256 devices in a mesh: expert: 8 (over x, z_lo), shard: 32 (over z_hi, y, core).
Axes of the slice: x: 4, y: 4, z: 8 (z_hi: 4, z_lo: 2; z = z_hi * 2 + z_lo), core: 2. Of those that a mesh axis runs over, the one named last changes fastest.
Arguments:
- tokens: bfloat16 [2048, 4096], P(('expert', 'shard')), may hold values from -6 to 6
- expert_ids: int32 [2048, 2], P(('expert', 'shard')), may hold values from 0 to 7, all different within a row; in each aligned block of 8 rows (0 to 7, 8 to 15, ...) at most 4 rows name the same one
- route_weights: float32 [2048, 2], P(('expert', 'shard')), may hold values from 0.1 to 1
- w_gate: bfloat16 [8, 4096, 12288], P('expert', None, 'shard'), may hold values from -0.09375 to 0.09375
- w_up: bfloat16 [8, 4096, 12288], P('expert', None, 'shard'), may hold values from -0.09375 to 0.09375
- w_down: bfloat16 [8, 12288, 4096], P('expert', 'shard'), may hold values from -0.0546875 to 0.0546875
Outputs:
- combined: bfloat16 [2048, 4096], P(('expert', 'shard'))
The draws below stay inside these ranges and needn't reach their ends.
Inputs may be any that keep to these rules, and one draw needn't show every extreme that they name: `expert_ids`: each row names 2 different experts. Among the rows of one device no expert is named by more than 4 rows, a bound that some block reaches on some devices.
All inputs are finite; a program needn't handle non-finite values.
Results may differ from the reference program's by a relative error of at most 0.015.
Values may be sent and summed in bfloat16 or wider, within the bound.
A program may use at most 128 MiB of HBM per device.

```python
import math
import jax
import jax.numpy as jnp
import numpy as np
from jax import lax

D = 4096
FF = 12288
TOP = 2
TOK_DEV = 8
EXPERTS = 8
CAP = 4
TOKENS = 2048
ROWS = 1024
N_SHARD = 32


def levels(own_key, extent, cuts, smallest, top_value):
    level, own = 1.0, jax.random.fold_in(own_key, 6)
    for position, shards_of in cuts:
        steps = jnp.exp(jax.random.uniform(jax.random.fold_in(own, position), (shards_of,), jnp.float32, smallest / len(cuts), top_value / len(cuts)))
        level = level * jnp.repeat(steps, extent[position] // shards_of).reshape([-1 if axis == position else 1 for axis in range(len(extent))])
    return level


def routed_block(rng, own, number, rows, number_of, top, most, lean):
    order = jax.random.permutation(rng, number_of)
    heavy_load, usual = portions_of(number_of, rows * top, most, lean, True), portions_of(number_of, rows * top, most, lean, False)
    places = jnp.arange(number_of)

    def named(tallies, offset_by):
        used = int((tallies > 0).sum())
        fixed = max(1, used // 4)
        passed = fixed + (places - fixed + offset_by * (used - fixed)) % max(1, number_of - fixed)
        return jnp.zeros((number_of,), jnp.int32).at[order[jnp.where(places < fixed, places, passed)]].set(jnp.asarray(tallies, jnp.int32))

    tallies = jnp.where(number % 4 == 0, named(heavy_load, number // 4), named(usual, number - number // 4 - 1))
    mixed = jax.random.permutation(jax.random.fold_in(own, 3), number_of)
    donor, taker = mixed[0:number_of // 2 * 2:2], mixed[1:number_of // 2 * 2:2]
    margin = jnp.minimum(tallies[donor] - 1, most - tallies[taker]) // 2
    margin = jnp.where((donor == order[0]) | (taker == order[0]) | (tallies[taker] == 0), 0, jnp.maximum(margin, 0))
    passed = jax.random.randint(jax.random.fold_in(own, 4), (number_of // 2,), 0, 1 << 20) % (margin + 1)
    tallies = tallies.at[donor].add(-passed).at[taker].add(passed)
    members = jnp.searchsorted(jnp.cumsum(tallies), jnp.arange(rows * top), side="right").astype(jnp.int32)
    table = members.reshape(top, rows).T
    table = table[jax.random.permutation(jax.random.fold_in(own, 1), rows)]
    offset_by = jax.random.randint(jax.random.fold_in(own, 2), (rows, 1), 0, top)
    return jnp.take_along_axis(table, (jnp.arange(top)[None, :] + offset_by) % top, axis=1)


def portions_of(count, total, limit, slope, full):
    loads = [(1 << 20) // math.isqrt(grade ** slope) + 1 for grade in range(1, count + 1)]
    largest = limit if full else min(limit, max(-(-total // count), total * loads[0] // sum(loads)))
    least = 1 if total - largest >= count - 1 else 0
    given, rest = [largest] + [least] * (count - 1), total - largest - least * (count - 1)
    while rest > 0:
        candidates = [i for i in range(1, count) if given[i] < largest] or [i for i in range(1, count) if given[i] < limit]
        mass, remaining = sum([loads[i] for i in candidates]), rest
        for i in candidates:
            extra = min(limit - given[i], max(1, remaining * loads[i] // mass), rest)
            given[i] = given[i] + extra
            rest = rest - extra
    return np.array(given)


def scatter_about(rng, dims, width, most, cuts=(), kind=jnp.bfloat16):
    gain = levels(rng, dims, cuts, -0.22, 0.18) if cuts else 1.0
    entries = jax.random.normal(rng, dims, jnp.float32) * width * gain
    return jnp.minimum(jnp.maximum(entries, -most), most).astype(kind)


def setup_inputs(seed: int = 0) -> dict:
    key_list = jax.random.split(jax.random.key(seed), 7)
    tokens = scatter_about(key_list[0], (TOKENS, D), 1.0, 6.0, ((0, 256),))
    expert_ids_keys = jax.random.split(jax.random.fold_in(key_list[1], 1), TOKENS // TOK_DEV)
    expert_ids_turns = jax.random.permutation(jax.random.fold_in(key_list[1], 3), TOKENS // TOK_DEV)
    expert_ids = jax.vmap(lambda own, number: routed_block(jax.random.fold_in(key_list[1], 2), own, number, TOK_DEV, EXPERTS, TOP, CAP, 2))(expert_ids_keys, expert_ids_turns).reshape((TOKENS, TOP))
    route_weights = jnp.clip(0.1 + 0.9 * jax.random.uniform(key_list[2], (TOKENS, TOP), jnp.float32) ** levels(key_list[2], (TOKENS, TOP), ((0, 256),), -0.2, 0.2), 0.1, 1.0)
    w_gate = scatter_about(key_list[3], (EXPERTS, D, FF), D ** -0.5, 0.09375, ((0, 8), (2, 32)))
    w_up = scatter_about(key_list[4], (EXPERTS, D, FF), D ** -0.5, 0.09375, ((0, 8), (2, 32)))
    w_down = scatter_about(key_list[5], (EXPERTS, FF, D), FF ** -0.5, 0.0546875, ((0, 8), (1, 32)))
    return {"tokens": tokens, "expert_ids": expert_ids, "route_weights": route_weights, "w_gate": w_gate, "w_up": w_up, "w_down": w_down}


def reference(tokens, expert_ids, route_weights, w_gate, w_up, w_down):
    token_count = tokens.shape[0]
    model_width = tokens.shape[1]
    row_limit = min(token_count, ROWS)
    group_width = w_down.shape[1] // N_SHARD
    combined = jnp.zeros((token_count, model_width), jnp.float32)
    for expert in range(w_gate.shape[0]):
        matched = expert_ids == expert
        scaling = jnp.sum(jnp.where(matched, route_weights, jnp.zeros_like(route_weights)), axis=1)
        routed = jnp.any(matched, axis=1)
        ranking = jnp.where(routed, 0, 1).astype(jnp.int32)
        picked = jnp.argsort(ranking, stable=True)[:row_limit].astype(jnp.int32)
        chosen = tokens[picked]
        gate_proj = jnp.dot(chosen, w_gate[expert], preferred_element_type=jnp.float32)
        up_proj = jnp.dot(chosen, w_up[expert], preferred_element_type=jnp.float32)
        hidden = (jax.nn.silu(gate_proj) * up_proj).astype(jnp.bfloat16)
        hidden_groups = hidden.reshape(row_limit, N_SHARD, group_width).transpose(1, 0, 2)
        down_groups = w_down[expert].reshape(N_SHARD, group_width, model_width)

        def add_group(total, pair):
            part_hidden, part_down = pair
            partial_value = jnp.dot(part_hidden, part_down, preferred_element_type=jnp.float32)
            rounded = lax.optimization_barrier(partial_value.astype(jnp.bfloat16))
            return total + rounded.astype(jnp.float32), None

        start = jnp.zeros((row_limit, model_width), jnp.float32)
        outputs, _ = lax.scan(add_group, start, (hidden_groups, down_groups))
        combined = combined.at[picked].add(outputs * scaling[picked][:, None])
    return combined.astype(jnp.bfloat16)
```

```python
import jax
import jax.numpy as jnp
from jax import lax
from jax.experimental import pallas as pl
from jax.experimental.pallas import tpu as pltpu
from jax.sharding import PartitionSpec as P

MESH = pl.DeviceIdType.MESH
BF = jnp.bfloat16
F32 = jnp.float32
NX, NY, NZ = 4, 4, 8
ORDER = (0, 1, 7, 2, 6, 3, 5, 4)
PLACE = {dz: divmod(p, 2) for p, dz in enumerate(ORDER)}
GROUPS = 4


def kernel(
    tok_ref, ids_ref, rw_ref, wg_ref, wu_ref, wd_ref, out_ref,
    xtok, xinfo, zsend, rows, wg, wu, wd, hid, part, fwd, fin, zsum, ret, mix, xsend, xown, xret,
    x_s, x_r, i_s, i_r, z_s, z_r, a_s, a_r, f_s, f_r, c_s, c_r, b_s, b_r, o_s, o_r, wl, w_s, w_r,
):
    width = tok_ref.shape[1]
    own_hidden = wg_ref.shape[2]
    e = lax.axis_index("expert")
    s = lax.axis_index("shard")
    x, z = e // 2, 2 * (s // 8) + e % 2
    y, c = (s // 2) % NY, s % 2

    def device(dx, dy, dz, dc=0):
        xx, yy, zz = (x + dx) % NX, (y + dy) % NY, (z + dz) % NZ
        return (2 * xx + zz % 2, (zz // 2) * 8 + yy * 2 + (c + dc) % 2)

    def remote(src, dst, send, recv, to):
        copy = pltpu.make_async_remote_copy(
            src_ref=src, dst_ref=dst, send_sem=send, recv_sem=recv, device_id=to, device_id_type=MESH
        )
        copy.start()
        return copy

    sent = []

    cols = pl.ds(0, own_hidden)
    far = pl.ds(own_hidden, own_hidden)
    loads = [
        pltpu.make_async_copy(wg_ref.at[0], wg.at[:, cols], wl.at[0]),
        pltpu.make_async_copy(wu_ref.at[0], wu.at[:, cols], wl.at[1]),
        pltpu.make_async_copy(wd_ref.at[0], wd.at[cols], wl.at[2]),
    ]
    for load in loads:
        load.start()

    barrier = pltpu.get_barrier_semaphore()
    peers = [device(k, 0, 0) for k in range(1, NX)] + [device(0, 0, k) for k in range(1, NZ)]
    peers += [device(0, 1, 0), device(0, 3, 0), device(0, 0, 0, 1)]
    for peer in peers:
        pl.semaphore_signal(barrier, inc=1, device_id=peer, device_id_type=MESH)

    lane = lax.broadcasted_iota(jnp.int32, (2, 128), 1)
    ids = ids_ref[...].astype(F32)
    rw = rw_ref[...]
    ids_wide = jnp.zeros((2, 128), F32)
    rw_wide = jnp.zeros((2, 128), F32)
    for t in range(8):
        ids_wide = jnp.where(lane % 8 == t, ids[:, t : t + 1], ids_wide)
        rw_wide = jnp.where(lane % 8 == t, rw[:, t : t + 1], rw_wide)
    xinfo[0] = jnp.concatenate([ids_wide, rw_wide, jnp.zeros((4, 128), F32)], axis=0)
    xtok[0] = tok_ref[...]

    pl.semaphore_wait(barrier, len(peers))

    info_in, tok_in = [], []
    for k in (1, 3, 2):
        info_in.append(remote(xinfo.at[0], xinfo.at[NX - k], i_s.at[k - 1], i_r.at[k - 1], device(k, 0, 0)))
        tok_in.append(remote(tok_ref, xtok.at[NX - k], x_s.at[k - 1], x_r.at[k - 1], device(k, 0, 0)))
    sent += info_in + tok_in

    partner = device(0, 0, 0, 1)
    weights_in = [
        remote(wg_ref.at[0], wg.at[:, far], w_s.at[0], w_r.at[0], partner),
        remote(wu_ref.at[0], wu.at[:, far], w_s.at[1], w_r.at[1], partner),
        remote(wd_ref.at[0], wd.at[far], w_s.at[2], w_r.at[2], partner),
    ]
    sent += weights_in

    for copy in info_in:
        copy.wait_recv()
    n_rows = 32
    lane = lax.broadcasted_iota(jnp.int32, (1, 128), 1)
    routes = []
    for k in range(4):
        v = jnp.zeros((1, 128), F32)
        for k2 in range(NX):
            v = jnp.where(lane // 8 == k2, xinfo[k2, k : k + 1, :], v)
        routes.append(v)
    id0, id1, w0, w1 = (jnp.broadcast_to(v, (n_rows, 128)) for v in routes)
    row = lax.broadcasted_iota(jnp.int32, (n_rows, 128), 0)
    lane = lax.broadcasted_iota(jnp.int32, (n_rows, 128), 1)
    e_other = e + 1 - 2 * (e % 2)
    wanted = jnp.where(row < 16, jnp.full((n_rows, 128), e), jnp.full((n_rows, 128), e_other)).astype(F32)
    first = id0 == wanted
    member = (first | (id1 == wanted)) & ((row // 4) % 4 == lane // 8)
    a = lax.broadcasted_iota(jnp.int32, (128, 128), 0)
    b = lax.broadcasted_iota(jnp.int32, (128, 128), 1)
    before = jnp.where((a < b) & (a // 8 == b // 8), 1.0, 0.0).astype(BF)
    position = jnp.dot(jnp.where(member, 1.0, 0.0).astype(BF), before, preferred_element_type=F32)
    chosen = member & (position == (row % 4).astype(F32))
    pick = jnp.where(chosen, 1.0, 0.0)
    weighted = jnp.where(chosen, jnp.where(first, w0, w1), 0.0)
    spread = jnp.concatenate([weighted] * 4, axis=0).T
    coarse = spread.astype(BF)
    fine = (spread - coarse.astype(F32)).astype(BF)
    mix[...] = jnp.concatenate([coarse[:32], fine[:32]], axis=0)

    for copy in tok_in:
        copy.wait_recv()
    pick = pick[:, :32].astype(BF)
    step = 1024
    for n in range(0, width, step):
        piece = jnp.dot(pick, xtok[:, :, n : n + step].reshape(32, step), preferred_element_type=F32).astype(BF)
        zsend[0, :, n : n + step] = piece[:16]
        zsend[1, :, n : n + step] = piece[16:]
        rows[0, 0, :, n : n + step] = piece[:16]

    z_in = {}
    for k in (7, 1, 6, 2, 5, 3, 4):
        dz = NZ - k
        g, i = PLACE[dz]
        z_in[dz] = remote(zsend.at[k % 2], rows.at[g, i], z_s.at[dz], z_r.at[dz], device(0, 0, k))
    sent += list(z_in.values())

    up, down = device(0, 1, 0), device(0, 3, 0)
    near_in = {}

    def spread_own(g):
        for i in range(2):
            p = 2 * g + i
            if p:
                z_in[ORDER[p]].wait_recv()
            src = zsend.at[0] if p == 0 else rows.at[g, i]
            near_in[p, 3] = remote(src, rows.at[g, 6 + i], a_s.at[0, p], a_r.at[2, p], up)
            near_in[p, 1] = remote(src, rows.at[g, 2 + i], a_s.at[1, p], a_r.at[0, p], down)
            sent.extend([near_in[p, 3], near_in[p, 1]])

    def spread_on(g):
        p = 2 * g
        near_in[p, 3].wait_recv()
        near_in[p, 2] = remote(rows.at[g, 6], rows.at[g, 4], a_s.at[2, p], a_r.at[1, p], up)
        p += 1
        near_in[p, 1].wait_recv()
        near_in[p, 2] = remote(rows.at[g, 3], rows.at[g, 5], a_s.at[2, p], a_r.at[1, p], down)
        sent.extend([near_in[p - 1, 2], near_in[p, 2]])

    def arrived(g):
        for p, ry in ((2 * g, 1), (2 * g + 1, 3), (2 * g, 2), (2 * g + 1, 2)):
            near_in[p, ry].wait_recv()

    def ffn(g):
        @pl.loop(0, 2 * own_hidden // 256)
        def _(n):
            at = pl.ds(pl.multiple_of(n * 256, 256), 256)
            block = rows[g].reshape(128, width)
            gate = jnp.dot(block, wg[:, at], preferred_element_type=F32)
            upward = jnp.dot(block, wu[:, at], preferred_element_type=F32)
            hid[:, at] = (gate / (1.0 + jnp.exp(-gate)) * upward).astype(BF)

        @pl.loop(0, width // 512)
        def _(n):
            at = pl.ds(pl.multiple_of(n * 512, 512), 512)
            out = jnp.dot(hid[...], wd[:, at], preferred_element_type=F32)
            part[g, :, :, at] = out.astype(BF).reshape(8, 16, 512)

    relay_in, final_in = {}, {}

    def reduce_first(g):
        relay_in[g, 0] = remote(part.at[g, 4], fwd.at[0, g], f_s.at[0, g], f_r.at[0, g], up)
        relay_in[g, 1] = remote(part.at[g, 5], fwd.at[1, g], f_s.at[1, g], f_r.at[1, g], down)
        final_in[g, 0, 1] = remote(part.at[g, 3], fin.at[0, g, 1], c_s.at[0, 2 * g + 1], c_r.at[0, 2 * g + 1], up)
        final_in[g, 1, 0] = remote(part.at[g, 6], fin.at[1, g, 0], c_s.at[1, 2 * g], c_r.at[1, 2 * g], down)

    def reduce_on(g):
        relay_in[g, 0].wait_recv()
        for n in range(0, width, step):
            at = slice(n, n + step)
            part[g, 2, :, at] = (part[g, 2, :, at].astype(F32) + fwd[0, g, :, at].astype(F32)).astype(BF)
        final_in[g, 0, 0] = remote(part.at[g, 2], fin.at[0, g, 0], c_s.at[0, 2 * g], c_r.at[0, 2 * g], up)
        relay_in[g, 1].wait_recv()
        for n in range(0, width, step):
            at = slice(n, n + step)
            part[g, 7, :, at] = (part[g, 7, :, at].astype(F32) + fwd[1, g, :, at].astype(F32)).astype(BF)
        final_in[g, 1, 1] = remote(part.at[g, 7], fin.at[1, g, 1], c_s.at[1, 2 * g + 1], c_r.at[1, 2 * g + 1], down)

    back_in = {}

    def finish(g):
        for i in (1, 0) if g % 2 else (0, 1):
            final_in[g, 0, i].wait_recv()
            final_in[g, 1, i].wait_recv()
            dz = ORDER[2 * g + i]
            for n in range(0, width, step):
                at = slice(n, n + step)
                total = part[g, i, :, at].astype(F32) + fin[0, g, i, :, at].astype(F32) + fin[1, g, i, :, at].astype(F32)
                if dz:
                    zsum[g, i, :, at] = total.astype(BF)
                else:
                    ret[0, :, at] = total.astype(BF)
            if dz:
                slot = NZ - dz
                back_in[slot] = remote(zsum.at[g, i], ret.at[slot], b_s.at[slot], b_r.at[slot], device(0, 0, dz))

    spread_own(0)
    spread_own(1)
    spread_on(0)
    for load in loads:
        load.wait()
    arrived(0)
    for copy in weights_in:
        copy.wait_recv()
    ffn(0)
    reduce_first(0)
    spread_on(1)
    spread_own(2)
    arrived(1)
    ffn(1)
    reduce_first(1)
    spread_on(2)
    spread_own(3)
    spread_on(3)
    arrived(2)
    ffn(2)
    reduce_first(2)
    arrived(3)
    ffn(3)
    reduce_first(3)
    reduce_on(0)
    reduce_on(1)
    finish(0)
    reduce_on(2)
    finish(1)
    reduce_on(3)
    finish(2)
    finish(3)
    sent += list(relay_in.values()) + list(final_in.values()) + list(back_in.values())

    for copy in back_in.values():
        copy.wait_recv()
    for n in range(0, width, step):
        at = slice(n, n + step)
        both = jnp.dot(mix[...], ret[:, :, at].reshape(128, step), preferred_element_type=F32)
        total = both[:32] + both[32:]
        for k in range(1, NX):
            xsend[k - 1, :, at] = total[8 * k : 8 * k + 8].astype(BF)
        xown[:, at] = total[:8]
    x_back = []
    for k in (1, 3, 2):
        x_back.append(remote(xsend.at[k - 1], xret.at[NX - k - 1], o_s.at[k - 1], o_r.at[k - 1], device(k, 0, 0)))
    sent += x_back
    for copy in x_back:
        copy.wait_recv()
    for n in range(0, width, step):
        at = slice(n, n + step)
        total = xown[:, at]
        for k in range(1, NX):
            total = total + xret[k - 1, :, at].astype(F32)
        out_ref[:, at] = total.astype(BF)
    for copy in sent:
        copy.wait_send()


def shards(tokens, expert_ids, route_weights, w_gate, w_up, w_down):
    block, width = tokens.shape
    hidden = w_gate.shape[2]
    dma = pltpu.SemaphoreType.DMA
    vmem = pl.BlockSpec(memory_space=pltpu.VMEM)
    hbm = pl.BlockSpec(memory_space=pl.ANY)
    return pl.pallas_call(
        kernel,
        out_shape=jax.ShapeDtypeStruct((block, width), BF),
        in_specs=[vmem, vmem, vmem, hbm, hbm, hbm],
        out_specs=vmem,
        scratch_shapes=[
            pltpu.VMEM((NX, block, width), BF),
            pltpu.VMEM((NX, 8, 128), F32),
            pltpu.VMEM((2, 16, width), BF),
            pltpu.VMEM((GROUPS, 8, 16, width), BF),
            pltpu.VMEM((width, 2 * hidden), BF),
            pltpu.VMEM((width, 2 * hidden), BF),
            pltpu.VMEM((2 * hidden, width), BF),
            pltpu.VMEM((128, 2 * hidden), BF),
            pltpu.VMEM((GROUPS, 8, 16, width), BF),
            pltpu.VMEM((2, GROUPS, 16, width), BF),
            pltpu.VMEM((2, GROUPS, 2, 16, width), BF),
            pltpu.VMEM((GROUPS, 2, 16, width), BF),
            pltpu.VMEM((NZ, 16, width), BF),
            pltpu.VMEM((64, 128), BF),
            pltpu.VMEM((3, block, width), BF),
            pltpu.VMEM((block, width), F32),
            pltpu.VMEM((3, block, width), BF),
            dma((3,)), dma((3,)), dma((3,)), dma((3,)),
            dma((8,)), dma((8,)),
            dma((3, 8)), dma((3, 8)),
            dma((2, 4)), dma((2, 4)), dma((2, 8)), dma((2, 8)),
            dma((8,)), dma((8,)),
            dma((3,)), dma((3,)),
            dma((3,)), dma((3,)), dma((3,)),
        ],
        compiler_params=pltpu.CompilerParams(
            collective_id=0, has_side_effects=True, vmem_limit_bytes=62 * 1024 * 1024
        ),
    )(tokens, expert_ids.T, route_weights.T, w_gate, w_up, w_down)


def solution(mesh):
    placed = (
        P(("expert", "shard"), None),
        P(("expert", "shard"), None),
        P(("expert", "shard"), None),
        P("expert", None, "shard"),
        P("expert", None, "shard"),
        P("expert", "shard", None),
    )
    return jax.shard_map(
        shards, mesh=mesh, in_specs=placed, out_specs=P(("expert", "shard"), None), check_vma=False
    )
```

```python
import jax
import jax.numpy as jnp
from jax import lax
from jax.experimental import pallas as pl
from jax.experimental.pallas import tpu as pltpu
from jax.sharding import PartitionSpec as P

MESH = pl.DeviceIdType.MESH
BF = jnp.bfloat16
F32 = jnp.float32
NX, NY, NZ = 4, 4, 8
ORDER = (0, 1, 7, 2, 6, 3, 5, 4)
PLACE = {dz: divmod(p, 2) for p, dz in enumerate(ORDER)}
GROUPS = 4
PARTS = 4


def kernel(
    tok_ref, ids_ref, rw_ref, wg_ref, wu_ref, wd_ref, out_ref,
    xtok, xinfo, zsend, rows, wg, wu, wd, hid, part, fwd, fin, zsum, ret, mix,
    x_s, x_r, i_s, i_r, z_s, z_r, a_s, a_r, f_s, f_r, c_s, c_r, b_s, b_r, wl, w_s, w_r,
):
    width = tok_ref.shape[1]
    own_hidden = wg_ref.shape[2]
    e = lax.axis_index("expert")
    s = lax.axis_index("shard")
    x, z = e // 2, 2 * (s // 8) + e % 2
    y, c = (s // 2) % NY, s % 2

    def device(dx, dy, dz, dc=0):
        xx, yy, zz = (x + dx) % NX, (y + dy) % NY, (z + dz) % NZ
        return (2 * xx + zz % 2, (zz // 2) * 8 + yy * 2 + (c + dc) % 2)

    def remote(src, dst, send, recv, to):
        copy = pltpu.make_async_remote_copy(
            src_ref=src, dst_ref=dst, send_sem=send, recv_sem=recv, device_id=to, device_id_type=MESH
        )
        copy.start()
        return copy

    sent = []

    cols = pl.ds(0, own_hidden)
    far = pl.ds(own_hidden, own_hidden)
    loads = [
        pltpu.make_async_copy(wg_ref.at[0], wg.at[:, cols], wl.at[0]),
        pltpu.make_async_copy(wu_ref.at[0], wu.at[:, cols], wl.at[1]),
        pltpu.make_async_copy(wd_ref.at[0], wd.at[cols], wl.at[2]),
    ]
    for load in loads:
        load.start()

    barrier = pltpu.get_barrier_semaphore()
    peers = [device(k, 0, 0) for k in range(1, NX)] + [device(0, 0, k) for k in (1, 2, 6, 7)]
    peers += [device(0, 1, 0), device(0, 3, 0), device(0, 0, 0, 1)]
    for peer in peers:
        pl.semaphore_signal(barrier, inc=1, device_id=peer, device_id_type=MESH)

    lane = lax.broadcasted_iota(jnp.int32, (2, 128), 1)
    ids = ids_ref[...].astype(F32)
    rw = rw_ref[...]
    ids_wide = jnp.zeros((2, 128), F32)
    rw_wide = jnp.zeros((2, 128), F32)
    for t in range(8):
        ids_wide = jnp.where(lane % 8 == t, ids[:, t : t + 1], ids_wide)
        rw_wide = jnp.where(lane % 8 == t, rw[:, t : t + 1], rw_wide)
    xinfo[0] = jnp.concatenate([ids_wide, rw_wide, jnp.zeros((4, 128), F32)], axis=0)
    xtok[0] = tok_ref[...]

    pl.semaphore_wait(barrier, len(peers))

    info_in, tok_in = [], []
    for k in (1, 3, 2):
        info_in.append(remote(xinfo.at[0], xinfo.at[NX - k], i_s.at[k - 1], i_r.at[k - 1], device(k, 0, 0)))
        tok_in.append(remote(tok_ref, xtok.at[NX - k], x_s.at[k - 1], x_r.at[k - 1], device(k, 0, 0)))
    sent += info_in + tok_in

    partner = device(0, 0, 0, 1)
    weights_in = []

    def weight_parts(n):
        for m in range(len(weights_in), len(weights_in) + n):
            w, k = m % 3, m // 3
            src, dst = ((wg_ref, wg), (wu_ref, wu), (wd_ref, wd))[w]
            size = src.shape[1] // PARTS
            at = pl.ds(k * size, size)
            to = dst.at[pl.ds(own_hidden + k * size, size)] if w == 2 else dst.at[at, far]
            weights_in.append(remote(src.at[0, at], to, w_s.at[w, k], w_r.at[w, k], partner))

    weight_parts(6)

    for copy in info_in:
        copy.wait_recv()
    n_rows = 32
    lane = lax.broadcasted_iota(jnp.int32, (1, 128), 1)
    routes = []
    for k in range(2):
        v = jnp.zeros((1, 128), F32)
        for k2 in range(NX):
            v = jnp.where(lane // 8 == k2, xinfo[k2, k : k + 1, :], v)
        routes.append(v)
    id0, id1 = (jnp.broadcast_to(v, (n_rows, 128)) for v in routes)
    row = lax.broadcasted_iota(jnp.int32, (n_rows, 128), 0)
    lane = lax.broadcasted_iota(jnp.int32, (n_rows, 128), 1)
    e_other = e + 1 - 2 * (e % 2)
    wanted = jnp.where(row < 16, jnp.full((n_rows, 128), e), jnp.full((n_rows, 128), e_other)).astype(F32)
    member = ((id0 == wanted) | (id1 == wanted)) & ((row // 4) % 4 == lane // 8)
    a = lax.broadcasted_iota(jnp.int32, (128, 128), 0)
    b = lax.broadcasted_iota(jnp.int32, (128, 128), 1)
    before = jnp.where((a < b) & (a // 8 == b // 8), 1.0, 0.0).astype(BF)
    position = jnp.dot(jnp.where(member, 1.0, 0.0).astype(BF), before, preferred_element_type=F32)
    chosen = member & (position == (row % 4).astype(F32))
    pick = jnp.where(chosen, 1.0, 0.0)

    for copy in tok_in:
        copy.wait_recv()
    pick = pick[:, :32].astype(BF)
    step = 1024
    for n in range(0, width, step):
        piece = jnp.dot(pick, xtok[:, :, n : n + step].reshape(32, step), preferred_element_type=F32).astype(BF)
        zsend[0, :, n : n + step] = piece[:16]
        zsend[1, :, n : n + step] = piece[16:]
        rows[0, 0, :, n : n + step] = piece[:16]

    z_in = {}

    def send_z(dz, src, sem, at=None):
        g, i = PLACE[dz]
        dst = rows.at[g, i] if at is None else rows.at[g, i, :, at]
        hop = (1, -1, 2, -2)[(7, 1, 6, 2).index(dz)] if dz in (7, 1, 6, 2) else (2 if sem in (5, 8) else -2)
        copy = remote(src, dst, z_s.at[sem], z_r.at[sem], device(0, 0, hop % NZ))
        z_in.setdefault(dz, []).append(copy)
        sent.append(copy)

    for dz in (1, 7, 2, 6):
        send_z(dz, zsend.at[dz % 2], dz)

    def pass_z(dz):
        g, i = PLACE[dz]
        if dz in (1, 7):
            send_z({1: 3, 7: 5}[dz], rows.at[g, i], {1: 3, 7: 5}[dz])
        if dz in (2, 6):
            at = pl.ds(0 if dz == 2 else width // 2, width // 2)
            send_z(4, rows.at[g, i, :, at], {2: 4, 6: 8}[dz], at)

    up, down = device(0, 1, 0), device(0, 3, 0)
    near_in = {}

    def spread_own(p):
        g, i = divmod(p, 2)
        dz = ORDER[p]
        for copy in z_in.get(dz, ()):
            copy.wait_recv()
        pass_z(dz)
        src = zsend.at[0] if p == 0 else rows.at[g, i]
        near_in[p, 3] = remote(src, rows.at[g, 6 + i], a_s.at[0, p], a_r.at[2, p], up)
        near_in[p, 1] = remote(src, rows.at[g, 2 + i], a_s.at[1, p], a_r.at[0, p], down)
        sent.extend([near_in[p, 3], near_in[p, 1]])

    def spread_on(g):
        p = 2 * g
        near_in[p, 3].wait_recv()
        near_in[p, 2] = remote(rows.at[g, 6], rows.at[g, 4], a_s.at[2, p], a_r.at[1, p], up)
        p += 1
        near_in[p, 1].wait_recv()
        near_in[p, 2] = remote(rows.at[g, 3], rows.at[g, 5], a_s.at[2, p], a_r.at[1, p], down)
        sent.extend([near_in[p - 1, 2], near_in[p, 2]])

    def arrived(g):
        for p, ry in ((2 * g, 1), (2 * g + 1, 3), (2 * g, 2), (2 * g + 1, 2)):
            near_in[p, ry].wait_recv()

    def ffn(g):
        @pl.loop(0, 2 * own_hidden // 256)
        def _(n):
            at = pl.ds(pl.multiple_of(n * 256, 256), 256)
            block = rows[g].reshape(128, width)
            gate = jnp.dot(block, wg[:, at], preferred_element_type=F32)
            upward = jnp.dot(block, wu[:, at], preferred_element_type=F32)
            hid[:, at] = (gate / (1.0 + jnp.exp(-gate)) * upward).astype(BF)

        @pl.loop(0, width // 512)
        def _(n):
            at = pl.ds(pl.multiple_of(n * 512, 512), 512)
            out = jnp.dot(hid[...], wd[:, at], preferred_element_type=F32)
            part[g, :, :, at] = out.astype(BF).reshape(8, 16, 512)

    relay_in, final_in = {}, {}

    def reduce_first(g):
        relay_in[g, 0] = remote(part.at[g, 4], fwd.at[0, g], f_s.at[0, g], f_r.at[0, g], up)
        relay_in[g, 1] = remote(part.at[g, 5], fwd.at[1, g], f_s.at[1, g], f_r.at[1, g], down)
        final_in[g, 0, 1] = remote(part.at[g, 3], fin.at[0, g, 1], c_s.at[0, 2 * g + 1], c_r.at[0, 2 * g + 1], up)
        final_in[g, 1, 0] = remote(part.at[g, 6], fin.at[1, g, 0], c_s.at[1, 2 * g], c_r.at[1, 2 * g], down)

    def reduce_on(g):
        relay_in[g, 0].wait_recv()
        for n in range(0, width, step):
            at = slice(n, n + step)
            part[g, 2, :, at] = (part[g, 2, :, at].astype(F32) + fwd[0, g, :, at].astype(F32)).astype(BF)
        final_in[g, 0, 0] = remote(part.at[g, 2], fin.at[0, g, 0], c_s.at[0, 2 * g], c_r.at[0, 2 * g], up)
        relay_in[g, 1].wait_recv()
        for n in range(0, width, step):
            at = slice(n, n + step)
            part[g, 7, :, at] = (part[g, 7, :, at].astype(F32) + fwd[1, g, :, at].astype(F32)).astype(BF)
        final_in[g, 1, 1] = remote(part.at[g, 7], fin.at[1, g, 1], c_s.at[1, 2 * g + 1], c_r.at[1, 2 * g + 1], down)

    row = lax.broadcasted_iota(jnp.int32, (32, 96), 0)
    col = lax.broadcasted_iota(jnp.int32, (32, 96), 1)
    fold = jnp.where(((row // 4) % 2 == col // 48) & (row // 8 * 4 + row % 4 == col % 16), 1.0, 0.0).astype(BF)
    back_in = {}
    half = width // 2

    def finish(g):
        for i in (1, 0):
            final_in[g, 0, i].wait_recv()
            final_in[g, 1, i].wait_recv()
            dz = ORDER[2 * g + i]
            for n in range(0, half, step):
                terms = [
                    ref[:, m + n : m + n + step]
                    for m in (0, half)
                    for ref in (part.at[g, i], fin.at[0, g, i], fin.at[1, g, i])
                ]
                total = jnp.dot(fold, jnp.concatenate(terms, axis=0), preferred_element_type=F32).astype(BF)
                for k in range(NX):
                    if dz or k:
                        zsum[g, i, k, :, n : n + step] = total[8 * k : 8 * k + 8]
                    else:
                        ret[0, 0, :, n : n + step] = total[:8]
            for k in (2, 1, 3, 0):
                if dz or k:
                    at = ((NZ - dz) % NZ, (NX - k) % NX)
                    back_in[at] = remote(zsum.at[g, i, k], ret.at[at[0], at[1]], b_s.at[at[0], at[1]], b_r.at[at[0], at[1]], device(k, 0, dz))

    row = lax.broadcasted_iota(jnp.int32, (256, 128), 0)
    lane = lax.broadcasted_iota(jnp.int32, (256, 128), 1)
    wanted = (2 * ((x + (row // 8) % 4) % NX) + (z + row // 32) % 2).astype(F32)
    id0, id1, w0, w1 = (jnp.broadcast_to(xinfo[0, k : k + 1, :], (256, 128)) for k in range(4))
    first = id0 == wanted
    member = first | (id1 == wanted)
    position = jnp.dot(jnp.where(member, 1.0, 0.0).astype(BF), before, preferred_element_type=F32)
    chosen = member & (position == (row % 4).astype(F32)) & (lane // 8 == (row // 4) % 2)
    spread = jnp.where(chosen, jnp.where(first, w0, w1), 0.0).T
    coarse = spread.astype(BF)
    fine = (spread - coarse.astype(F32)).astype(BF)

    spread_own(0)
    weight_parts(3)
    mix[...] = jnp.concatenate([coarse[:16], fine[:16]], axis=0)
    spread_own(1)
    spread_own(2)
    weight_parts(3)
    spread_on(0)
    spread_own(3)
    spread_own(4)
    for load in loads:
        load.wait()
    arrived(0)
    for copy in weights_in:
        copy.wait_recv()
    ffn(0)
    spread_on(1)
    spread_own(5)
    spread_own(6)
    arrived(1)
    ffn(1)
    spread_on(2)
    spread_own(7)
    arrived(2)
    ffn(2)
    spread_on(3)
    reduce_first(2)
    arrived(3)
    ffn(3)
    reduce_on(2)
    reduce_first(3)
    reduce_on(3)
    reduce_first(1)
    reduce_first(0)
    finish(2)
    reduce_on(1)
    finish(3)
    reduce_on(0)
    finish(1)
    finish(0)
    sent += weights_in + list(relay_in.values()) + list(final_in.values()) + list(back_in.values())

    for copy in back_in.values():
        copy.wait_recv()
    for n in range(0, half, step):
        both = jnp.dot(mix[...], ret[:, :, :, n : n + step].reshape(256, step), preferred_element_type=F32)
        total = (both[:16] + both[16:]).astype(BF)
        out_ref[:, n : n + step] = total[:8]
        out_ref[:, half + n : half + n + step] = total[8:]
    for copy in sent:
        copy.wait_send()


def shards(tokens, expert_ids, route_weights, w_gate, w_up, w_down):
    block, width = tokens.shape
    hidden = w_gate.shape[2]
    dma = pltpu.SemaphoreType.DMA
    vmem = pl.BlockSpec(memory_space=pltpu.VMEM)
    hbm = pl.BlockSpec(memory_space=pl.ANY)
    return pl.pallas_call(
        kernel,
        out_shape=jax.ShapeDtypeStruct((block, width), BF),
        in_specs=[vmem, vmem, vmem, hbm, hbm, hbm],
        out_specs=vmem,
        scratch_shapes=[
            pltpu.VMEM((NX, block, width), BF),
            pltpu.VMEM((NX, 8, 128), F32),
            pltpu.VMEM((2, 16, width), BF),
            pltpu.VMEM((GROUPS, 8, 16, width), BF),
            pltpu.VMEM((width, 2 * hidden), BF),
            pltpu.VMEM((width, 2 * hidden), BF),
            pltpu.VMEM((2 * hidden, width), BF),
            pltpu.VMEM((128, 2 * hidden), BF),
            pltpu.VMEM((GROUPS, 8, 16, width), BF),
            pltpu.VMEM((2, GROUPS, 16, width), BF),
            pltpu.VMEM((2, GROUPS, 2, 16, width), BF),
            pltpu.VMEM((GROUPS, 2, NX, 8, width // 2), BF),
            pltpu.VMEM((NZ, NX, 8, width // 2), BF),
            pltpu.VMEM((32, 256), BF),
            dma((3,)), dma((3,)), dma((3,)), dma((3,)),
            dma((9,)), dma((9,)),
            dma((3, 8)), dma((3, 8)),
            dma((2, 4)), dma((2, 4)), dma((2, 8)), dma((2, 8)),
            dma((NZ, NX)), dma((NZ, NX)),
            dma((3,)), dma((3, PARTS)), dma((3, PARTS)),
        ],
        compiler_params=pltpu.CompilerParams(
            collective_id=0, has_side_effects=True, vmem_limit_bytes=62 * 1024 * 1024
        ),
    )(tokens, expert_ids.T, route_weights.T, w_gate, w_up, w_down)


def solution(mesh):
    placed = (
        P(("expert", "shard"), None),
        P(("expert", "shard"), None),
        P(("expert", "shard"), None),
        P("expert", None, "shard"),
        P("expert", None, "shard"),
        P("expert", "shard", None),
    )
    return jax.shard_map(
        shards, mesh=mesh, in_specs=placed, out_specs=P(("expert", "shard"), None), check_vma=False
    )
```

```python
import jax
import jax.numpy as jnp
from jax import lax
from jax.experimental import pallas as pl
from jax.experimental.pallas import tpu as pltpu
from jax.sharding import PartitionSpec as P

MESH = pl.DeviceIdType.MESH
BF = jnp.bfloat16
F32 = jnp.float32
NX, NY, NZ = 4, 4, 8
ORDER = (0, 1, 7, 2, 5, 4, 6, 3)
PLACE = {dz: divmod(p, 2) for p, dz in enumerate(ORDER)}
GROUPS = 4
STRAIGHT = (0, 7, 1, 6)
SUMMED = (3, 4, 2, 5)
PARTS = 4


def kernel(
    tok_ref, ids_ref, rw_ref, wg_ref, wu_ref, wd_ref, out_ref,
    xtok, xinfo, zsend, rows, wg, wu, wd, hid, part, fwd, fin, zsum, ret, mix, yinfo, zback, near, ymix, ysum, yown, yret,
    x_s, x_r, i_s, i_r, z_s, z_r, a_s, a_r, f_s, f_r, c_s, c_r, b_s, b_r, n_s, n_r, j_s, j_r, y_s, y_r, wl, w_s, w_r,
):
    width = tok_ref.shape[1]
    own_hidden = wg_ref.shape[2]
    e = lax.axis_index("expert")
    s = lax.axis_index("shard")
    x, z = e // 2, 2 * (s // 8) + e % 2
    y, c = (s // 2) % NY, s % 2

    def device(dx, dy, dz, dc=0):
        xx, yy, zz = (x + dx) % NX, (y + dy) % NY, (z + dz) % NZ
        return (2 * xx + zz % 2, (zz // 2) * 8 + yy * 2 + (c + dc) % 2)

    def remote(src, dst, send, recv, to):
        copy = pltpu.make_async_remote_copy(
            src_ref=src, dst_ref=dst, send_sem=send, recv_sem=recv, device_id=to, device_id_type=MESH
        )
        copy.start()
        return copy

    sent = []

    cols = pl.ds(0, own_hidden)
    far = pl.ds(own_hidden, own_hidden)
    loads = [
        pltpu.make_async_copy(wg_ref.at[0], wg.at[:, cols], wl.at[0]),
        pltpu.make_async_copy(wu_ref.at[0], wu.at[:, cols], wl.at[1]),
        pltpu.make_async_copy(wd_ref.at[0], wd.at[cols], wl.at[2]),
    ]
    for load in loads:
        load.start()

    barrier = pltpu.get_barrier_semaphore()
    peers = [device(k, 0, 0) for k in range(1, NX)] + [device(0, 0, k) for k in (1, 2, 6, 7)]
    peers += [device(0, k, 0) for k in range(1, NY)] + [device(0, 0, 0, 1)]
    for peer in peers:
        pl.semaphore_signal(barrier, inc=1, device_id=peer, device_id_type=MESH)

    lane = lax.broadcasted_iota(jnp.int32, (2, 128), 1)
    ids = ids_ref[...].astype(F32)
    rw = rw_ref[...]
    ids_wide = jnp.zeros((2, 128), F32)
    rw_wide = jnp.zeros((2, 128), F32)
    for t in range(8):
        ids_wide = jnp.where(lane % 8 == t, ids[:, t : t + 1], ids_wide)
        rw_wide = jnp.where(lane % 8 == t, rw[:, t : t + 1], rw_wide)
    xinfo[0] = jnp.concatenate([ids_wide, rw_wide, jnp.zeros((4, 128), F32)], axis=0)
    xtok[0] = tok_ref[...]

    pl.semaphore_wait(barrier, len(peers))

    info_in, tok_in = [], []
    for k in (1, 3, 2):
        info_in.append(remote(xinfo.at[0], xinfo.at[NX - k], i_s.at[k - 1], i_r.at[k - 1], device(k, 0, 0)))
        tok_in.append(remote(tok_ref, xtok.at[NX - k], x_s.at[k - 1], x_r.at[k - 1], device(k, 0, 0)))
    yinfo_in = [
        remote(xinfo.at[0], yinfo.at[NY - k], j_s.at[k - 1], j_r.at[k - 1], device(0, k, 0)) for k in (1, 3, 2)
    ]
    sent += info_in + tok_in + yinfo_in

    partner = device(0, 0, 0, 1)
    weights_in = []

    def weight_parts(n):
        for m in range(len(weights_in), len(weights_in) + n):
            w, k = m % 3, m // 3
            src, dst = ((wg_ref, wg), (wu_ref, wu), (wd_ref, wd))[w]
            size = src.shape[1] // PARTS
            at = pl.ds(k * size, size)
            to = dst.at[pl.ds(own_hidden + k * size, size)] if w == 2 else dst.at[at, far]
            weights_in.append(remote(src.at[0, at], to, w_s.at[w, k], w_r.at[w, k], partner))

    weight_parts(6)

    for copy in info_in:
        copy.wait_recv()
    n_rows = 32
    lane = lax.broadcasted_iota(jnp.int32, (1, 128), 1)
    routes = []
    for k in range(2):
        v = jnp.zeros((1, 128), F32)
        for k2 in range(NX):
            v = jnp.where(lane // 8 == k2, xinfo[k2, k : k + 1, :], v)
        routes.append(v)
    id0, id1 = (jnp.broadcast_to(v, (n_rows, 128)) for v in routes)
    row = lax.broadcasted_iota(jnp.int32, (n_rows, 128), 0)
    lane = lax.broadcasted_iota(jnp.int32, (n_rows, 128), 1)
    e_other = e + 1 - 2 * (e % 2)
    wanted = jnp.where(row < 16, jnp.full((n_rows, 128), e), jnp.full((n_rows, 128), e_other)).astype(F32)
    member = ((id0 == wanted) | (id1 == wanted)) & ((row // 4) % 4 == lane // 8)
    a = lax.broadcasted_iota(jnp.int32, (128, 128), 0)
    b = lax.broadcasted_iota(jnp.int32, (128, 128), 1)
    before = jnp.where((a < b) & (a // 8 == b // 8), 1.0, 0.0).astype(BF)
    position = jnp.dot(jnp.where(member, 1.0, 0.0).astype(BF), before, preferred_element_type=F32)
    chosen = member & (position == (row % 4).astype(F32))
    pick = jnp.where(chosen, 1.0, 0.0)

    for copy in tok_in:
        copy.wait_recv()
    pick = pick[:, :32].astype(BF)
    step = 1024
    for n in range(0, width, step):
        piece = jnp.dot(pick, xtok[:, :, n : n + step].reshape(32, step), preferred_element_type=F32).astype(BF)
        zsend[0, :, n : n + step] = piece[:16]
        zsend[1, :, n : n + step] = piece[16:]
        rows[0, 0, :, n : n + step] = piece[:16]

    z_in = {}

    def send_z(dz, src, sem, at=None):
        g, i = PLACE[dz]
        dst = rows.at[g, i] if at is None else rows.at[g, i, :, at]
        hop = (1, -1, 2, -2)[(7, 1, 6, 2).index(dz)] if dz in (7, 1, 6, 2) else (2 if sem in (5, 8) else -2)
        copy = remote(src, dst, z_s.at[sem], z_r.at[sem], device(0, 0, hop % NZ))
        z_in.setdefault(dz, []).append(copy)
        sent.append(copy)

    for dz in (1, 7, 2, 6):
        send_z(dz, zsend.at[dz % 2], dz)

    def pass_z(dz):
        g, i = PLACE[dz]
        if dz in (1, 7):
            send_z({1: 3, 7: 5}[dz], rows.at[g, i], {1: 3, 7: 5}[dz])
        if dz in (2, 6):
            at = pl.ds(0 if dz == 2 else width // 2, width // 2)
            send_z(4, rows.at[g, i, :, at], {2: 4, 6: 8}[dz], at)

    up, down = device(0, 1, 0), device(0, 3, 0)
    near_in = {}

    def spread_own(p):
        g, i = divmod(p, 2)
        dz = ORDER[p]
        for copy in z_in.get(dz, ()):
            copy.wait_recv()
        pass_z(dz)
        src = zsend.at[0] if p == 0 else rows.at[g, i]
        near_in[p, 3] = remote(src, rows.at[g, 6 + i], a_s.at[0, p], a_r.at[2, p], up)
        near_in[p, 1] = remote(src, rows.at[g, 2 + i], a_s.at[1, p], a_r.at[0, p], down)
        sent.extend([near_in[p, 3], near_in[p, 1]])

    def spread_on(p):
        g, i = divmod(p, 2)
        came, to, ry = (3, up, 6) if i == 0 else (1, down, 3)
        near_in[p, came].wait_recv()
        near_in[p, 2] = remote(rows.at[g, ry], rows.at[g, 4 + i], a_s.at[2, p], a_r.at[1, p], to)
        sent.append(near_in[p, 2])

    def arrived(g):
        for p, ry in ((2 * g, 1), (2 * g + 1, 3), (2 * g, 2), (2 * g + 1, 2)):
            near_in[p, ry].wait_recv()

    def ffn_up(g):
        @pl.loop(0, 2 * own_hidden // 256)
        def _(n):
            at = pl.ds(pl.multiple_of(n * 256, 256), 256)
            block = rows[g].reshape(128, width)
            gate = jnp.dot(block, wg[:, at], preferred_element_type=F32)
            upward = jnp.dot(block, wu[:, at], preferred_element_type=F32)
            hid[:, at] = (gate / (1.0 + jnp.exp(-gate)) * upward).astype(BF)

    def ffn_down(g):
        @pl.loop(0, width // 512)
        def _(n):
            at = pl.ds(pl.multiple_of(n * 512, 512), 512)
            out = jnp.dot(hid[...], wd[:, at], preferred_element_type=F32)
            part[g, :, :, at] = out.astype(BF).reshape(8, 16, 512)

    relay_in, final_in = {}, {}

    def reduce_first(g):
        relay_in[g, 0] = remote(part.at[g, 4], fwd.at[0, g - 2], f_s.at[0, g - 2], f_r.at[0, g - 2], up)
        relay_in[g, 1] = remote(part.at[g, 5], fwd.at[1, g - 2], f_s.at[1, g - 2], f_r.at[1, g - 2], down)
        final_in[g, 0, 1] = remote(part.at[g, 3], fin.at[0, g - 2, 1], c_s.at[0, 2 * g - 3], c_r.at[0, 2 * g - 3], up)
        final_in[g, 1, 0] = remote(part.at[g, 6], fin.at[1, g - 2, 0], c_s.at[1, 2 * g - 4], c_r.at[1, 2 * g - 4], down)

    def reduce_on(g):
        relay_in[g, 0].wait_recv()
        for n in range(0, width, step):
            at = slice(n, n + step)
            part[g, 2, :, at] = (part[g, 2, :, at].astype(F32) + fwd[0, g - 2, :, at].astype(F32)).astype(BF)
        final_in[g, 0, 0] = remote(part.at[g, 2], fin.at[0, g - 2, 0], c_s.at[0, 2 * g - 4], c_r.at[0, 2 * g - 4], up)
        relay_in[g, 1].wait_recv()
        for n in range(0, width, step):
            at = slice(n, n + step)
            part[g, 7, :, at] = (part[g, 7, :, at].astype(F32) + fwd[1, g - 2, :, at].astype(F32)).astype(BF)
        final_in[g, 1, 1] = remote(part.at[g, 7], fin.at[1, g - 2, 1], c_s.at[1, 2 * g - 3], c_r.at[1, 2 * g - 3], down)

    row = lax.broadcasted_iota(jnp.int32, (32, 96), 0)
    col = lax.broadcasted_iota(jnp.int32, (32, 96), 1)
    fold = jnp.where(((row // 4) % 2 == col // 48) & (row // 8 * 4 + row % 4 == col % 16), 1.0, 0.0).astype(BF)
    back_in = {}
    half = width // 2

    def finish(g):
        for i in (1, 0):
            final_in[g, 0, i].wait_recv()
            final_in[g, 1, i].wait_recv()
            dz = ORDER[2 * g + i]
            slot = SUMMED.index(NZ - dz)
            for n in range(0, half, step):
                terms = [
                    ref[:, m + n : m + n + step]
                    for m in (0, half)
                    for ref in (part.at[g, i], fin.at[0, g - 2, i], fin.at[1, g - 2, i])
                ]
                total = jnp.dot(fold, jnp.concatenate(terms, axis=0), preferred_element_type=F32).astype(BF)
                for k in range(NX):
                    zsum[g - 2, i, k, :, n : n + step] = total[8 * k : 8 * k + 8]
            for k in (2, 1, 3, 0):
                to = (NX - k) % NX
                back_in[slot, to] = remote(zsum.at[g - 2, i, k], ret.at[slot, to], b_s.at[slot, to], b_r.at[slot, to], device(k, 0, dz))

    row = lax.broadcasted_iota(jnp.int32, (32, 32), 0)
    col = lax.broadcasted_iota(jnp.int32, (32, 32), 1)
    fold_one = jnp.where(((row // 4) % 2 == col // 16) & (row // 8 * 4 + row % 4 == col % 16), 1.0, 0.0).astype(BF)
    straight_in = {}

    def go_back(g):
        for i in range(2):
            dz = ORDER[2 * g + i]
            slot = STRAIGHT.index((NZ - dz) % NZ)
            for ry in range(NY):
                for n in range(0, half, step):
                    terms = [part[g, 2 * ry + i, :, m + n : m + n + step] for m in (0, half)]
                    moved = jnp.dot(fold_one, jnp.concatenate(terms, axis=0), preferred_element_type=F32).astype(BF)
                    for k in range(NX):
                        if dz or k:
                            zback[g, i, k, ry, :, n : n + step] = moved[8 * k : 8 * k + 8]
                        else:
                            near[0, 0, ry, :, n : n + step] = moved[:8]
            for k in (2, 1, 3, 0):
                to = (NX - k) % NX
                if dz or k:
                    straight_in[slot, to] = remote(zback.at[g, i, k], near.at[slot, to], n_s.at[slot, to], n_r.at[slot, to], device(k, 0, dz))

    def token_mix(info, flip):
        row = lax.broadcasted_iota(jnp.int32, (128, 128), 0)
        lane = lax.broadcasted_iota(jnp.int32, (128, 128), 1)
        wanted = (2 * ((x + (row // 8) % 4) % NX) + (z + (row // 32 + 1) // 2 + flip) % 2).astype(F32)
        id0, id1, w0, w1 = (jnp.broadcast_to(info[k : k + 1, :], (128, 128)) for k in range(4))
        first = id0 == wanted
        member = first | (id1 == wanted)
        position = jnp.dot(jnp.where(member, 1.0, 0.0).astype(BF), before, preferred_element_type=F32)
        chosen = member & (position == (row % 4).astype(F32)) & (lane // 8 == (row // 4) % 2)
        spread = jnp.where(chosen, jnp.where(first, w0, w1), 0.0).T
        coarse = spread.astype(BF)
        fine = (spread - coarse.astype(F32)).astype(BF)
        return jnp.concatenate([coarse[:16], fine[:16]], axis=0)

    y_back = []

    def sum_straight():
        for copy in straight_in.values():
            copy.wait_recv()
        for ry in (2, 1, 3, 0):
            for n in range(0, half, step):
                both = jnp.dot(ymix[ry], near[:, :, ry, :, n : n + step].reshape(128, step), preferred_element_type=F32)
                total = both[:16] + both[16:]
                for m in range(2):
                    at = slice(m * half + n, m * half + n + step)
                    if ry:
                        ysum[ry - 1, :, at] = total[8 * m : 8 * m + 8].astype(BF)
                    else:
                        yown[:, at] = total[8 * m : 8 * m + 8]
            if ry:
                y_back.append(remote(ysum.at[ry - 1], yret.at[NY - ry - 1], y_s.at[ry - 1], y_r.at[ry - 1], device(0, ry, 0)))

    spread_own(0)
    weight_parts(3)
    mix[...] = token_mix(xinfo[0], 1)
    spread_own(1)
    spread_own(2)
    weight_parts(3)
    spread_on(0)
    spread_on(1)
    spread_own(3)
    spread_own(6)
    for load in loads:
        load.wait()
    arrived(0)
    for copy in weights_in:
        copy.wait_recv()
    ffn_up(0)
    spread_on(2)
    spread_own(4)
    ffn_down(0)
    spread_on(3)
    go_back(0)
    spread_own(5)
    spread_own(7)
    arrived(1)
    ffn_up(1)
    spread_on(4)
    spread_on(6)
    spread_on(5)
    ffn_down(1)
    go_back(1)
    spread_on(7)
    for copy in yinfo_in:
        copy.wait_recv()
    ymix[0] = token_mix(xinfo[0], 0)
    for k in range(1, NY):
        ymix[k] = token_mix(yinfo[k], 0)
    arrived(2)
    ffn_up(2)
    ffn_down(2)
    reduce_first(2)
    arrived(3)
    ffn_up(3)
    ffn_down(3)
    reduce_on(2)
    reduce_first(3)
    finish(2)
    reduce_on(3)
    finish(3)
    sum_straight()
    sent += weights_in + list(relay_in.values()) + list(final_in.values()) + list(back_in.values())
    sent += list(straight_in.values()) + y_back

    for copy in y_back:
        copy.wait_recv()
    for copy in back_in.values():
        copy.wait_recv()
    for n in range(0, half, step):
        both = jnp.dot(mix[...], ret[:, :, :, n : n + step].reshape(128, step), preferred_element_type=F32)
        total = both[:16] + both[16:]
        for m in range(2):
            at = slice(m * half + n, m * half + n + step)
            rest = yown[:, at]
            for k in range(NY - 1):
                rest = rest + yret[k, :, at].astype(F32)
            out_ref[:, at] = (total[8 * m : 8 * m + 8] + rest).astype(BF)
    for copy in sent:
        copy.wait_send()


def shards(tokens, expert_ids, route_weights, w_gate, w_up, w_down):
    block, width = tokens.shape
    hidden = w_gate.shape[2]
    dma = pltpu.SemaphoreType.DMA
    vmem = pl.BlockSpec(memory_space=pltpu.VMEM)
    hbm = pl.BlockSpec(memory_space=pl.ANY)
    return pl.pallas_call(
        kernel,
        out_shape=jax.ShapeDtypeStruct((block, width), BF),
        in_specs=[vmem, vmem, vmem, hbm, hbm, hbm],
        out_specs=vmem,
        scratch_shapes=[
            pltpu.VMEM((NX, block, width), BF),
            pltpu.VMEM((NX, 8, 128), F32),
            pltpu.VMEM((2, 16, width), BF),
            pltpu.VMEM((GROUPS, 8, 16, width), BF),
            pltpu.VMEM((width, 2 * hidden), BF),
            pltpu.VMEM((width, 2 * hidden), BF),
            pltpu.VMEM((2 * hidden, width), BF),
            pltpu.VMEM((128, 2 * hidden), BF),
            pltpu.VMEM((GROUPS, 8, 16, width), BF),
            pltpu.VMEM((2, 2, 16, width), BF),
            pltpu.VMEM((2, 2, 2, 16, width), BF),
            pltpu.VMEM((2, 2, NX, 8, width // 2), BF),
            pltpu.VMEM((4, NX, 8, width // 2), BF),
            pltpu.VMEM((32, 128), BF),
            pltpu.VMEM((NY, 8, 128), F32),
            pltpu.VMEM((2, 2, NX, NY, 8, width // 2), BF),
            pltpu.VMEM((4, NX, NY, 8, width // 2), BF),
            pltpu.VMEM((NY, 32, 128), BF),
            pltpu.VMEM((3, block, width), BF),
            pltpu.VMEM((block, width), F32),
            pltpu.VMEM((3, block, width), BF),
            dma((3,)), dma((3,)), dma((3,)), dma((3,)),
            dma((9,)), dma((9,)),
            dma((3, 8)), dma((3, 8)),
            dma((2, 2)), dma((2, 2)), dma((2, 4)), dma((2, 4)),
            dma((4, NX)), dma((4, NX)),
            dma((4, NX)), dma((4, NX)),
            dma((3,)), dma((3,)), dma((3,)), dma((3,)),
            dma((3,)), dma((3, PARTS)), dma((3, PARTS)),
        ],
        compiler_params=pltpu.CompilerParams(
            collective_id=0, has_side_effects=True, vmem_limit_bytes=62 * 1024 * 1024
        ),
    )(tokens, expert_ids.T, route_weights.T, w_gate, w_up, w_down)


def solution(mesh):
    placed = (
        P(("expert", "shard"), None),
        P(("expert", "shard"), None),
        P(("expert", "shard"), None),
        P("expert", None, "shard"),
        P("expert", None, "shard"),
        P("expert", "shard", None),
    )
    return jax.shard_map(
        shards, mesh=mesh, in_specs=placed, out_specs=P(("expert", "shard"), None), check_vma=False
    )
```

```python
import jax
import jax.numpy as jnp
from jax import lax
from jax.experimental import pallas as pl
from jax.experimental.pallas import tpu as pltpu
from jax.sharding import PartitionSpec as P

MESH = pl.DeviceIdType.MESH
BF = jnp.bfloat16
F32 = jnp.float32
NX, NY, NZ = 4, 4, 8
ORDER = (0, 1, 7, 2, 5, 4, 6, 3)
PLACE = {dz: divmod(p, 2) for p, dz in enumerate(ORDER)}
GROUPS = 4
STRAIGHT = (0, 7, 1, 6)
SUMMED = (3, 4, 2, 5)
PARTS = 4
POOL = 40
DOWN = 2048


def kernel(
    tok_ref, ids_ref, rw_ref, wg_ref, wu_ref, wd_ref, out_ref,
    xtok, xinfo, zsend, rows, wg, wu, wd, hid, part, fwd, fin, zsum, ret, mix, yinfo, zback, near, ymix, ysum, yown, yret, ids_in, rw_in,
    send, all_s, x_r, i_r, z_r, a_r, d_r, f_r, c_r, b_r, n_r, j_r, y_r, t_s, wl, w_r,
):
    width = tok_ref.shape[1]
    own = [
        pltpu.make_async_copy(ids_ref, ids_in, t_s.at[0]),
        pltpu.make_async_copy(rw_ref, rw_in, t_s.at[1]),
        pltpu.make_async_copy(tok_ref, xtok.at[0], t_s.at[2]),
    ]
    for copy in own:
        copy.start()
    own_hidden = wg_ref.shape[2]
    e = lax.axis_index("expert")
    s = lax.axis_index("shard")
    x, z = e // 2, 2 * (s // 8) + e % 2
    y, c = (s // 2) % NY, s % 2

    def device(dx, dy, dz, dc=0):
        xx, yy, zz = (x + dx) % NX, (y + dy) % NY, (z + dz) % NZ
        return (2 * xx + zz % 2, (zz // 2) * 8 + yy * 2 + (c + dc) % 2)

    sent = []

    def remote(src, dst, recv, to, own_send=None):
        n = len(sent)
        if own_send is None and n >= POOL:
            sent[n - POOL].wait_send()
        copy = pltpu.make_async_remote_copy(
            src_ref=src, dst_ref=dst, send_sem=send.at[n % POOL] if own_send is None else own_send, recv_sem=recv, device_id=to, device_id_type=MESH
        )
        copy.start()
        if own_send is None:
            sent.append(copy)
        return copy

    def landed(ref, sem):
        pltpu.make_async_copy(ref, ref, sem).wait()

    cols = pl.ds(0, own_hidden)
    far = pl.ds(own_hidden, own_hidden)
    loads = [
        pltpu.make_async_copy(wg_ref.at[0], wg.at[:, cols], wl.at[0]),
        pltpu.make_async_copy(wu_ref.at[0], wu.at[:, cols], wl.at[1]),
        pltpu.make_async_copy(wd_ref.at[0], wd.at[cols], wl.at[2]),
    ]

    barrier = pltpu.get_barrier_semaphore()
    peers = [device(k, 0, 0) for k in range(1, NX)] + [device(0, 0, k) for k in (1, 2, 6, 7)]
    peers += [device(0, k, 0) for k in range(1, NY)] + [device(0, 0, 0, 1)]
    for peer in peers:
        pl.semaphore_signal(barrier, inc=1, device_id=peer, device_id_type=MESH)

    for load in loads:
        load.start()
    for copy in own:
        copy.wait()

    lane = lax.broadcasted_iota(jnp.int32, (2, 128), 1)
    ids = ids_in[...].astype(F32)
    rw = rw_in[...]
    ids_wide = jnp.zeros((2, 128), F32)
    rw_wide = jnp.zeros((2, 128), F32)
    for t in range(8):
        ids_wide = jnp.where(lane % 8 == t, ids[:, t : t + 1], ids_wide)
        rw_wide = jnp.where(lane % 8 == t, rw[:, t : t + 1], rw_wide)
    xinfo[0] = jnp.concatenate([ids_wide, rw_wide, jnp.zeros((4, 128), F32)], axis=0)

    pl.semaphore_wait(barrier, len(peers))

    for k in (1, 3, 2):
        remote(xinfo.at[0], xinfo.at[NX - k], i_r.at[0], device(k, 0, 0))
    half = width // 2
    halves = (pl.ds(0, half), pl.ds(half, half))
    for h, at in enumerate(halves):
        for k in (1, 3, 2):
            remote(xtok.at[0, :, at], xtok.at[NX - k, :, at], x_r.at[h], device(k, 0, 0))
    for k in (1, 3, 2):
        remote(xinfo.at[0], yinfo.at[NY - k], j_r.at[0], device(0, k, 0))

    partner = device(0, 0, 0, 1)
    weights_in = []

    def weight_parts(n):
        for m in range(len(weights_in), len(weights_in) + n):
            w, k = m % 3, m // 3
            src, dst = ((wg_ref, wg), (wu_ref, wu), (wd_ref, wd))[w]
            size = src.shape[1] // PARTS
            at = pl.ds(k * size, size)
            to = dst.at[pl.ds(own_hidden + k * size, size)] if w == 2 else dst.at[at, far]
            weights_in.append(remote(src.at[0, at], to, w_r.at[w], partner))

    weight_parts(6)

    landed(xinfo.at[pl.ds(1, 3)], i_r.at[0])
    n_rows = 32
    lane = lax.broadcasted_iota(jnp.int32, (1, 128), 1)
    routes = []
    for k in range(2):
        v = jnp.zeros((1, 128), F32)
        for k2 in range(NX):
            v = jnp.where(lane // 8 == k2, xinfo[k2, k : k + 1, :], v)
        routes.append(v)
    id0, id1 = (jnp.broadcast_to(v, (n_rows, 128)) for v in routes)
    row = lax.broadcasted_iota(jnp.int32, (n_rows, 128), 0)
    lane = lax.broadcasted_iota(jnp.int32, (n_rows, 128), 1)
    e_other = e + 1 - 2 * (e % 2)
    wanted = jnp.where(row < 16, jnp.full((n_rows, 128), e), jnp.full((n_rows, 128), e_other)).astype(F32)
    member = ((id0 == wanted) | (id1 == wanted)) & ((row // 4) % 4 == lane // 8)
    a = lax.broadcasted_iota(jnp.int32, (128, 128), 0)
    b = lax.broadcasted_iota(jnp.int32, (128, 128), 1)
    before = jnp.where((a < b) & (a // 8 == b // 8), 1.0, 0.0).astype(BF)
    position = jnp.dot(jnp.where(member, 1.0, 0.0).astype(BF), before, preferred_element_type=F32)
    chosen = member & (position == (row % 4).astype(F32))
    pick = jnp.where(chosen, 1.0, 0.0)

    up, down = device(0, 1, 0), device(0, 3, 0)
    z_in, near_in = {}, {}

    def send_z(dz, src, sem, hop, at=None):
        g, i = PLACE[dz]
        dst = rows.at[g, i] if at is None else rows.at[g, i, :, at]
        z_in.setdefault(dz, []).append(remote(src, dst, z_r.at[sem], device(0, 0, hop % NZ)))

    def send_y(p, h=None):
        g, i = divmod(p, 2)
        src = rows.at[g, i] if p else zsend.at[0]
        to_up, to_down, n = rows.at[g, 6 + i], rows.at[g, 2 + i], p + 8 if h else p
        if h is not None:
            src, to_up, to_down = (ref.at[:, halves[h]] for ref in (src, to_up, to_down))
        near_in.setdefault((p, 3), []).append(remote(src, to_up, a_r.at[1, n], up))
        near_in.setdefault((p, 1), []).append(remote(src, to_down, a_r.at[0, n], down))

    pick = pick[:, :32].astype(BF)
    step = 1024
    for h, at in enumerate(halves):
        landed(xtok.at[pl.ds(1, 3), :, at], x_r.at[h])
        for n in range(h * half, h * half + half, step):
            piece = jnp.dot(pick, xtok[:, :, n : n + step].reshape(32, step), preferred_element_type=F32).astype(BF)
            zsend[0, :, n : n + step] = piece[:16]
            zsend[1, :, n : n + step] = piece[16:]
            rows[0, 0, :, n : n + step] = piece[:16]
        send_z(1, zsend.at[1, :, at], 1 + 8 * h, -1, at)
        send_z(7, zsend.at[1, :, at], 7 + 3 * h, 1, at)
        send_y(0, h)
    send_z(2, zsend.at[0], 2, -2)
    send_z(6, zsend.at[0], 6, 2)

    def pass_z(dz):
        g, i = PLACE[dz]
        hop = -2 if dz < 4 else 2
        if dz in (1, 7):
            send_z((dz - hop) % NZ, rows.at[g, i], (dz - hop) % NZ, hop)
        if dz in (2, 6):
            at = halves[dz // 4]
            send_z(4, rows.at[g, i, :, at], {2: 4, 6: 8}[dz], hop, at)

    def spread_own(p):
        dz = ORDER[p]
        for copy in z_in[dz]:
            copy.wait_recv()
        pass_z(dz)
        send_y(p)

    def spread_first():
        for h in range(2):
            for p in (1, 2):
                z_in[ORDER[p]][h].wait_recv()
                send_y(p, h)
                if h:
                    pass_z(ORDER[p])

    def spread_on(p):
        g, i = divmod(p, 2)
        came, to, ry = (3, up, 6) if i == 0 else (1, down, 3)
        for copy in near_in[p, came]:
            copy.wait_recv()
        remote(rows.at[g, ry], rows.at[g, 4 + i], d_r.at[g], to)

    def arrived(g):
        for p, ry in ((2 * g, 1), (2 * g + 1, 3)):
            for copy in near_in[p, ry]:
                copy.wait_recv()
        landed(rows.at[g, pl.ds(4, 2)], d_r.at[g])

    def ffn_up(g):
        for n in range(0, 2 * own_hidden, 256):
            at = pl.ds(n, 256)
            block = rows[g].reshape(128, width)
            gate = jnp.dot(block, wg[:, at], preferred_element_type=F32)
            upward = jnp.dot(block, wu[:, at], preferred_element_type=F32)
            hid[:, at] = (gate / (1.0 + jnp.exp(-gate)) * upward).astype(BF)

    def ffn_down(g):
        @pl.loop(0, width // DOWN)
        def _(n):
            at = pl.ds(pl.multiple_of(n * DOWN, DOWN), DOWN)
            out = jnp.dot(hid[...], wd[:, at], preferred_element_type=F32)
            part[g, :, :, at] = out.astype(BF).reshape(8, 16, DOWN)

    relay_in = {}

    def final(g, side, i, h):
        src = part.at[g, ((2, 3), (6, 7))[side][i], :, halves[h]]
        dst = fin.at[side, g - 2, i, :, halves[h]]
        at = 2 * (g - 2) + i
        remote(src, dst, c_r.at[at, h], (up, down)[side])

    def reduce_first(g):
        for h in range(2):
            for side in range(2):
                src, dst = part.at[g, 4 + side, :, halves[h]], fwd.at[side, g - 2, :, halves[h]]
                relay_in[g, side, h] = remote(src, dst, f_r.at[side, g - 2, h], (up, down)[side])
        for h in range(2):
            final(g, 0, 1, h)
            final(g, 1, 0, h)

    def reduce_on(g):
        for h in range(2):
            for side, ry in ((0, 2), (1, 7)):
                relay_in[g, side, h].wait_recv()
                for n in range(h * half, h * half + half, step):
                    at = slice(n, n + step)
                    part[g, ry, :, at] = (part[g, ry, :, at].astype(F32) + fwd[side, g - 2, :, at].astype(F32)).astype(BF)
                final(g, side, side, h)

    row = lax.broadcasted_iota(jnp.int32, (32, 96), 0)
    col = lax.broadcasted_iota(jnp.int32, (32, 96), 1)
    fold = jnp.where(((row // 4) % 2 == col // 48) & (row // 8 * 4 + row % 4 == col % 16), 1.0, 0.0).astype(BF)

    def finish(g):
        for h in range(2):
            for i in (1, 0):
                landed(fin.at[:, g - 2, i, :, halves[h]], c_r.at[2 * (g - 2) + i, h])
                dz = ORDER[2 * g + i]
                slot = SUMMED.index(NZ - dz)
                terms = [
                    ref[:, m : m + step]
                    for m in (h * half, h * half + step)
                    for ref in (part.at[g, i], fin.at[0, g - 2, i], fin.at[1, g - 2, i])
                ]
                total = jnp.dot(fold, jnp.concatenate(terms, axis=0), preferred_element_type=F32).astype(BF)
                at = pl.ds(h * step, step)
                for k in range(NX):
                    zsum[g - 2, i, k, :, h * step : h * step + step] = total[8 * k : 8 * k + 8]
                for k in (2, 1, 3, 0):
                    to = (NX - k) % NX
                    remote(zsum.at[g - 2, i, k, :, at], ret.at[slot, to, :, at], b_r.at[0], device(k, 0, dz), all_s.at[3])

    row = lax.broadcasted_iota(jnp.int32, (32, 32), 0)
    col = lax.broadcasted_iota(jnp.int32, (32, 32), 1)
    fold_one = jnp.where(((row // 4) % 2 == col // 16) & (row // 8 * 4 + row % 4 == col % 16), 1.0, 0.0).astype(BF)

    def go_back(g):
        for i in range(2):
            dz = ORDER[2 * g + i]
            slot = STRAIGHT.index((NZ - dz) % NZ)
            for ry in range(NY):
                for n in range(0, half, step):
                    terms = [part[g, 2 * ry + i, :, 2 * n + m : 2 * n + m + step] for m in (0, step)]
                    moved = jnp.dot(fold_one, jnp.concatenate(terms, axis=0), preferred_element_type=F32).astype(BF)
                    for k in range(NX):
                        if dz or k:
                            zback[g, i, k, ry, :, n : n + step] = moved[8 * k : 8 * k + 8]
                        else:
                            near[0, 0, ry, :, n : n + step] = moved[:8]
            for k in (2, 1, 3, 0):
                to = (NX - k) % NX
                if dz or k:
                    remote(zback.at[g, i, k], near.at[slot, to], n_r.at[min(slot, 1)], device(k, 0, dz), all_s.at[i if g == 0 else 2])

    def token_mix(info, flip):
        row = lax.broadcasted_iota(jnp.int32, (128, 128), 0)
        lane = lax.broadcasted_iota(jnp.int32, (128, 128), 1)
        wanted = (2 * ((x + (row // 8) % 4) % NX) + (z + (row // 32 + 1) // 2 + flip) % 2).astype(F32)
        id0, id1, w0, w1 = (jnp.broadcast_to(info[k : k + 1, :], (128, 128)) for k in range(4))
        first = id0 == wanted
        member = first | (id1 == wanted)
        position = jnp.dot(jnp.where(member, 1.0, 0.0).astype(BF), before, preferred_element_type=F32)
        chosen = member & (position == (row % 4).astype(F32)) & (lane // 8 == (row // 4) % 2)
        spread = jnp.where(chosen, jnp.where(first, w0, w1), 0.0).T
        coarse = spread.astype(BF)
        fine = (spread - coarse.astype(F32)).astype(BF)
        return jnp.concatenate([coarse[:16], fine[:16]], axis=0)

    def sum_straight():
        landed(near.at[0, pl.ds(1, 3)], n_r.at[0])
        landed(near.at[pl.ds(1, 3)], n_r.at[1])
        for ry in (2, 1, 3, 0):
            for n in range(0, half, step):
                both = jnp.dot(ymix[ry], near[:, :, ry, :, n : n + step].reshape(128, step), preferred_element_type=F32)
                total = both[:16] + both[16:]
                for m in range(2):
                    at = slice(2 * n + m * step, 2 * n + m * step + step)
                    if ry:
                        ysum[ry - 1, :, at] = total[8 * m : 8 * m + 8].astype(BF)
                    else:
                        yown[:, at] = total[8 * m : 8 * m + 8]
            if ry:
                remote(ysum.at[ry - 1], yret.at[NY - ry - 1], y_r.at[0], device(0, ry, 0), all_s.at[4])

    weight_parts(3)
    mix[...] = token_mix(xinfo[0], 1)
    spread_first()
    weight_parts(3)
    spread_on(0)
    spread_on(1)
    spread_own(3)
    spread_own(6)
    for load in loads:
        load.wait()
    arrived(0)
    for n, ref in enumerate((wg.at[:, far], wu.at[:, far], wd.at[far])):
        landed(ref, w_r.at[n])
    ffn_up(0)
    spread_on(2)
    spread_own(4)
    ffn_down(0)
    spread_on(3)
    go_back(0)
    spread_own(5)
    spread_own(7)
    arrived(1)
    ffn_up(1)
    spread_on(4)
    spread_on(6)
    spread_on(5)
    ffn_down(1)
    go_back(1)
    spread_on(7)
    landed(yinfo.at[pl.ds(1, 3)], j_r.at[0])
    ymix[0] = token_mix(xinfo[0], 0)
    for k in range(1, NY):
        ymix[k] = token_mix(yinfo[k], 0)
    arrived(2)
    ffn_up(2)
    ffn_down(2)
    reduce_first(2)
    arrived(3)
    ffn_up(3)
    ffn_down(3)
    reduce_on(2)
    reduce_first(3)
    finish(2)
    reduce_on(3)
    finish(3)
    sum_straight()

    landed(yret, y_r.at[0])
    landed(ret, b_r.at[0])
    for n in range(0, half, step):
        both = jnp.dot(mix[...], ret[:, :, :, n : n + step].reshape(128, step), preferred_element_type=F32)
        total = both[:16] + both[16:]
        for m in range(2):
            at = slice(2 * n + m * step, 2 * n + m * step + step)
            rest = yown[:, at]
            for k in range(NY - 1):
                rest = rest + yret[k, :, at].astype(F32)
            out_ref[:, at] = (total[8 * m : 8 * m + 8] + rest).astype(BF)
    for copy in sent[-POOL:]:
        copy.wait_send()
    for n, ref in enumerate((zback.at[0, 0, pl.ds(1, 3)], zback.at[0, 1], zback.at[1], zsum, ysum)):
        landed(ref, all_s.at[n])


def shards(tokens, expert_ids, route_weights, w_gate, w_up, w_down):
    block, width = tokens.shape
    hidden = w_gate.shape[2]
    dma = pltpu.SemaphoreType.DMA
    vmem = pl.BlockSpec(memory_space=pltpu.VMEM)
    hbm = pl.BlockSpec(memory_space=pl.ANY)
    return pl.pallas_call(
        kernel,
        out_shape=jax.ShapeDtypeStruct((block, width), BF),
        in_specs=[hbm] * 6,
        out_specs=vmem,
        scratch_shapes=[
            pltpu.VMEM((NX, block, width), BF),
            pltpu.VMEM((NX, 8, 128), F32),
            pltpu.VMEM((2, 16, width), BF),
            pltpu.VMEM((GROUPS, 8, 16, width), BF),
            pltpu.VMEM((width, 2 * hidden), BF),
            pltpu.VMEM((width, 2 * hidden), BF),
            pltpu.VMEM((2 * hidden, width), BF),
            pltpu.VMEM((128, 2 * hidden), BF),
            pltpu.VMEM((GROUPS, 8, 16, width), BF),
            pltpu.VMEM((2, 2, 16, width), BF),
            pltpu.VMEM((2, 2, 2, 16, width), BF),
            pltpu.VMEM((2, 2, NX, 8, width // 2), BF),
            pltpu.VMEM((4, NX, 8, width // 2), BF),
            pltpu.VMEM((32, 128), BF),
            pltpu.VMEM((NY, 8, 128), F32),
            pltpu.VMEM((2, 2, NX, NY, 8, width // 2), BF),
            pltpu.VMEM((4, NX, NY, 8, width // 2), BF),
            pltpu.VMEM((NY, 32, 128), BF),
            pltpu.VMEM((3, block, width), BF),
            pltpu.VMEM((block, width), F32),
            pltpu.VMEM((3, block, width), BF),
            pltpu.VMEM((2, 8), jnp.int32),
            pltpu.VMEM((2, 8), F32),
            dma((POOL,)), dma((5,)),
            dma((2,)), dma((1,)),
            dma((11,)),
            dma((2, 11)), dma((4,)),
            dma((2, 2, 2)), dma((4, 2)),
            dma((1,)),
            dma((2,)),
            dma((1,)), dma((1,)),
            dma((3,)),
            dma((3,)), dma((3,)),
        ],
        compiler_params=pltpu.CompilerParams(
            collective_id=0, has_side_effects=True, vmem_limit_bytes=62 * 1024 * 1024
        ),
    )(tokens, expert_ids.T, route_weights.T, w_gate, w_up, w_down)


def solution(mesh):
    placed = (
        P(("expert", "shard"), None),
        P(("expert", "shard"), None),
        P(("expert", "shard"), None),
        P("expert", None, "shard"),
        P("expert", None, "shard"),
        P("expert", "shard", None),
    )
    return jax.shard_map(
        shards, mesh=mesh, in_specs=placed, out_specs=P(("expert", "shard"), None), check_vma=False
    )
```

```python
import jax
import jax.numpy as jnp
from jax import lax
from jax.experimental import pallas as pl
from jax.experimental.pallas import tpu as pltpu
from jax.sharding import PartitionSpec as P

MESH = pl.DeviceIdType.MESH
BF = jnp.bfloat16
F32 = jnp.float32
NX, NY, NZ = 4, 4, 8
ORDER = (0, 1, 7, 2, 5, 4, 6, 3)
PLACE = {dz: divmod(p, 2) for p, dz in enumerate(ORDER)}
GROUPS = 4
STRAIGHT = (0, 7, 1, 6)
SUMMED = (3, 4, 2, 5)
PARTS = 4
POOL = 32
DOWN = 2048


def kernel(
    tok_ref, ids_ref, rw_ref, wg_ref, wu_ref, wd_ref, out_ref,
    xtok, xinfo, zsend, rows, wg, wu, wd, hid, part, fwd, fin, zsum, ret, mix, yinfo, zback, near, ymix, ysum, yown, yret, ids_in, rw_in,
    send, all_s, x_r, i_r, z_r, a_r, d_r, f_r, c_r, b_r, n_r, j_r, y_r, t_s, wl, w_r,
):
    width = tok_ref.shape[1]
    own = [
        pltpu.make_async_copy(ids_ref, ids_in, t_s.at[0]),
        pltpu.make_async_copy(rw_ref, rw_in, t_s.at[1]),
        pltpu.make_async_copy(tok_ref, xtok.at[0], t_s.at[2]),
    ]
    for copy in own:
        copy.start()
    own_hidden = wg_ref.shape[2]
    e = lax.axis_index("expert")
    s = lax.axis_index("shard")
    x, z = e // 2, 2 * (s // 8) + e % 2
    y, c = (s // 2) % NY, s % 2

    def device(dx, dy, dz, dc=0):
        xx, yy, zz = (x + dx) % NX, (y + dy) % NY, (z + dz) % NZ
        return (2 * xx + zz % 2, (zz // 2) * 8 + yy * 2 + (c + dc) % 2)

    sent = []

    def remote(src, dst, recv, to, own_send=None):
        n = len(sent)
        if own_send is None and n >= POOL:
            sent[n - POOL].wait_send()
        copy = pltpu.make_async_remote_copy(
            src_ref=src, dst_ref=dst, send_sem=send.at[n % POOL] if own_send is None else own_send, recv_sem=recv, device_id=to, device_id_type=MESH
        )
        copy.start()
        if own_send is None:
            sent.append(copy)
        return copy

    def landed(ref, sem):
        pltpu.make_async_copy(ref, ref, sem).wait()

    cols = pl.ds(0, own_hidden)
    far = pl.ds(own_hidden, own_hidden)
    loads = [
        pltpu.make_async_copy(wg_ref.at[0], wg.at[:, cols], wl.at[0]),
        pltpu.make_async_copy(wu_ref.at[0], wu.at[:, cols], wl.at[1]),
        pltpu.make_async_copy(wd_ref.at[0], wd.at[cols], wl.at[2]),
    ]

    barrier = pltpu.get_barrier_semaphore()
    peers = [device(k, 0, 0) for k in range(1, NX)] + [device(0, 0, k) for k in (1, 2, 6, 7)]
    peers += [device(0, k, 0) for k in range(1, NY)] + [device(0, 0, 0, 1)]
    for peer in peers:
        pl.semaphore_signal(barrier, inc=1, device_id=peer, device_id_type=MESH)

    for load in loads:
        load.start()
    for copy in own:
        copy.wait()

    lane = lax.broadcasted_iota(jnp.int32, (2, 128), 1)
    ids = ids_in[...].astype(F32)
    rw = rw_in[...]
    ids_wide = jnp.zeros((2, 128), F32)
    rw_wide = jnp.zeros((2, 128), F32)
    for t in range(8):
        ids_wide = jnp.where(lane % 8 == t, ids[:, t : t + 1], ids_wide)
        rw_wide = jnp.where(lane % 8 == t, rw[:, t : t + 1], rw_wide)
    xinfo[0] = jnp.concatenate([ids_wide, rw_wide, jnp.zeros((4, 128), F32)], axis=0)

    pl.semaphore_wait(barrier, len(peers))

    for k in (1, 3, 2):
        remote(xinfo.at[0], xinfo.at[NX - k], i_r.at[0], device(k, 0, 0))
    half = width // 2
    halves = (pl.ds(0, half), pl.ds(half, half))
    for h, at in enumerate(halves):
        for k in (1, 3, 2):
            remote(xtok.at[0, :, at], xtok.at[NX - k, :, at], x_r.at[h], device(k, 0, 0))
    for k in (1, 3, 2):
        remote(xinfo.at[0], yinfo.at[NY - k], j_r.at[0], device(0, k, 0))

    partner = device(0, 0, 0, 1)
    weights_in = []

    def weight_parts(n):
        for m in range(len(weights_in), len(weights_in) + n):
            w, k = m % 3, m // 3
            src, dst = ((wg_ref, wg), (wu_ref, wu), (wd_ref, wd))[w]
            size = src.shape[1] // PARTS
            at = pl.ds(k * size, size)
            to = dst.at[pl.ds(own_hidden + k * size, size)] if w == 2 else dst.at[at, far]
            weights_in.append(remote(src.at[0, at], to, w_r.at[w], partner))

    weight_parts(6)

    landed(xinfo.at[pl.ds(1, 3)], i_r.at[0])
    n_rows = 32
    lane = lax.broadcasted_iota(jnp.int32, (1, 128), 1)
    routes = []
    for k in range(2):
        v = jnp.zeros((1, 128), F32)
        for k2 in range(NX):
            v = jnp.where(lane // 8 == k2, xinfo[k2, k : k + 1, :], v)
        routes.append(v)
    id0, id1 = (jnp.broadcast_to(v, (n_rows, 128)) for v in routes)
    row = lax.broadcasted_iota(jnp.int32, (n_rows, 128), 0)
    lane = lax.broadcasted_iota(jnp.int32, (n_rows, 128), 1)
    e_other = e + 1 - 2 * (e % 2)
    wanted = jnp.where(row < 16, jnp.full((n_rows, 128), e), jnp.full((n_rows, 128), e_other)).astype(F32)
    member = ((id0 == wanted) | (id1 == wanted)) & ((row // 4) % 4 == lane // 8)
    a = lax.broadcasted_iota(jnp.int32, (128, 128), 0)
    b = lax.broadcasted_iota(jnp.int32, (128, 128), 1)
    before = jnp.where((a < b) & (a // 8 == b // 8), 1.0, 0.0).astype(BF)
    position = jnp.dot(jnp.where(member, 1.0, 0.0).astype(BF), before, preferred_element_type=F32)
    chosen = member & (position == (row % 4).astype(F32))
    pick = jnp.where(chosen, 1.0, 0.0)

    up, down = device(0, 1, 0), device(0, 3, 0)
    z_in, near_in = {}, {}

    def send_z(dz, src, sem, hop, at=None):
        g, i = PLACE[dz]
        dst = rows.at[g, i] if at is None else rows.at[g, i, :, at]
        z_in.setdefault(dz, []).append(remote(src, dst, z_r.at[sem], device(0, 0, hop % NZ)))

    def send_y(p, h=None):
        g, i = divmod(p, 2)
        src = rows.at[g, i] if p else zsend.at[0]
        to_up, to_down, n = rows.at[g, 6 + i], rows.at[g, 2 + i], p + 8 if h else p
        if h is not None:
            src, to_up, to_down = (ref.at[:, halves[h]] for ref in (src, to_up, to_down))
        near_in.setdefault((p, 3), []).append(remote(src, to_up, a_r.at[1, n], up))
        near_in.setdefault((p, 1), []).append(remote(src, to_down, a_r.at[0, n], down))

    pick = pick[:, :32].astype(BF)
    step = 1024
    for h, at in enumerate(halves):
        landed(xtok.at[pl.ds(1, 3), :, at], x_r.at[h])
        for n in range(h * half, h * half + half, step):
            piece = jnp.dot(pick, xtok[:, :, n : n + step].reshape(32, step), preferred_element_type=F32).astype(BF)
            zsend[0, :, n : n + step] = piece[:16]
            zsend[1, :, n : n + step] = piece[16:]
            rows[0, 0, :, n : n + step] = piece[:16]
        send_z(1, zsend.at[1, :, at], 1 + 8 * h, -1, at)
        send_z(7, zsend.at[1, :, at], 7 + 3 * h, 1, at)
        send_y(0, h)
    send_z(2, zsend.at[0], 2, -2)
    send_z(6, zsend.at[0], 6, 2)

    def pass_z(dz):
        g, i = PLACE[dz]
        hop = -2 if dz < 4 else 2
        if dz in (1, 7):
            send_z((dz - hop) % NZ, rows.at[g, i], (dz - hop) % NZ, hop)
        if dz in (2, 6):
            at = halves[dz // 4]
            send_z(4, rows.at[g, i, :, at], {2: 4, 6: 8}[dz], hop, at)

    def spread_own(p):
        dz = ORDER[p]
        for copy in z_in[dz]:
            copy.wait_recv()
        pass_z(dz)
        send_y(p)

    def spread_first():
        for h in range(2):
            for p in (1, 2):
                z_in[ORDER[p]][h].wait_recv()
                send_y(p, h)
                if h:
                    pass_z(ORDER[p])

    def spread_on(p):
        g, i = divmod(p, 2)
        came, to, ry = (3, up, 6) if i == 0 else (1, down, 3)
        for copy in near_in[p, came]:
            copy.wait_recv()
        remote(rows.at[g, ry], rows.at[g, 4 + i], d_r.at[g], to)

    def arrived(g):
        for p, ry in ((2 * g, 1), (2 * g + 1, 3)):
            for copy in near_in[p, ry]:
                copy.wait_recv()
        landed(rows.at[g, pl.ds(4, 2)], d_r.at[g])

    def ffn_up(g):
        for n in range(0, 2 * own_hidden, 256):
            at = pl.ds(n, 256)
            block = rows[g].reshape(128, width)
            gate = jnp.dot(block, wg[:, at], preferred_element_type=F32)
            upward = jnp.dot(block, wu[:, at], preferred_element_type=F32)
            hid[:, at] = (gate / (1.0 + jnp.exp(-gate)) * upward).astype(BF)

    def ffn_down(g):
        @pl.loop(0, width // DOWN)
        def _(n):
            at = pl.ds(pl.multiple_of(n * DOWN, DOWN), DOWN)
            out = jnp.dot(hid[...], wd[:, at], preferred_element_type=F32)
            part[g, :, :, at] = out.astype(BF).reshape(8, 16, DOWN)

    relay_in = {}

    def final(g, side, i, h):
        src = part.at[g, ((2, 3), (6, 7))[side][i], :, halves[h]]
        dst = fin.at[side, g - 2, i, :, halves[h]]
        at = 2 * (g - 2) + i
        remote(src, dst, c_r.at[at, h], (up, down)[side])

    def down_and_reduce(g):
        for h in range(2):
            out = jnp.dot(hid[...], wd[:, halves[h]], preferred_element_type=F32)
            part[g, :, :, halves[h]] = out.astype(BF).reshape(8, 16, half)
            for side in range(2):
                src, dst = part.at[g, 4 + side, :, halves[h]], fwd.at[side, g - 2, :, halves[h]]
                relay_in[g, side, h] = remote(src, dst, f_r.at[side, g - 2, h], (up, down)[side])

    def reduce_first(g):
        for h in range(2):
            final(g, 0, 1, h)
            final(g, 1, 0, h)

    def reduce_on(g):
        for h in range(2):
            for side, ry in ((0, 2), (1, 7)):
                relay_in[g, side, h].wait_recv()
                for n in range(h * half, h * half + half, step):
                    at = slice(n, n + step)
                    part[g, ry, :, at] = (part[g, ry, :, at].astype(F32) + fwd[side, g - 2, :, at].astype(F32)).astype(BF)
                final(g, side, side, h)

    row = lax.broadcasted_iota(jnp.int32, (32, 96), 0)
    col = lax.broadcasted_iota(jnp.int32, (32, 96), 1)
    fold = jnp.where(((row // 4) % 2 == col // 48) & (row // 8 * 4 + row % 4 == col % 16), 1.0, 0.0).astype(BF)

    def finish(g):
        for h in range(2):
            for i in (1, 0):
                landed(fin.at[:, g - 2, i, :, halves[h]], c_r.at[2 * (g - 2) + i, h])
                dz = ORDER[2 * g + i]
                slot = SUMMED.index(NZ - dz)
                terms = [
                    ref[:, m : m + step]
                    for m in (h * half, h * half + step)
                    for ref in (part.at[g, i], fin.at[0, g - 2, i], fin.at[1, g - 2, i])
                ]
                total = jnp.dot(fold, jnp.concatenate(terms, axis=0), preferred_element_type=F32).astype(BF)
                at = pl.ds(h * step, step)
                for k in range(NX):
                    zsum[g - 2, i, k, :, h * step : h * step + step] = total[8 * k : 8 * k + 8]
                for k in (2, 1, 3, 0):
                    to = (NX - k) % NX
                    remote(zsum.at[g - 2, i, k, :, at], ret.at[slot, to, :, at], b_r.at[0], device(k, 0, dz), all_s.at[3])

    row = lax.broadcasted_iota(jnp.int32, (32, 32), 0)
    col = lax.broadcasted_iota(jnp.int32, (32, 32), 1)
    fold_one = jnp.where(((row // 4) % 2 == col // 16) & (row // 8 * 4 + row % 4 == col % 16), 1.0, 0.0).astype(BF)

    def go_back(g):
        for i in range(2):
            dz = ORDER[2 * g + i]
            slot = STRAIGHT.index((NZ - dz) % NZ)
            for ry in range(NY):
                for n in range(0, half, step):
                    terms = [part[g, 2 * ry + i, :, 2 * n + m : 2 * n + m + step] for m in (0, step)]
                    moved = jnp.dot(fold_one, jnp.concatenate(terms, axis=0), preferred_element_type=F32).astype(BF)
                    for k in range(NX):
                        if dz or k:
                            zback[g, i, k, ry, :, n : n + step] = moved[8 * k : 8 * k + 8]
                        else:
                            near[0, 0, ry, :, n : n + step] = moved[:8]
            for k in (2, 1, 3, 0):
                to = (NX - k) % NX
                if dz or k:
                    remote(zback.at[g, i, k], near.at[slot, to], n_r.at[min(slot, 1)], device(k, 0, dz), all_s.at[i if g == 0 else 2])

    def token_mix(info, flip):
        row = lax.broadcasted_iota(jnp.int32, (128, 128), 0)
        lane = lax.broadcasted_iota(jnp.int32, (128, 128), 1)
        wanted = (2 * ((x + (row // 8) % 4) % NX) + (z + (row // 32 + 1) // 2 + flip) % 2).astype(F32)
        id0, id1, w0, w1 = (jnp.broadcast_to(info[k : k + 1, :], (128, 128)) for k in range(4))
        first = id0 == wanted
        member = first | (id1 == wanted)
        position = jnp.dot(jnp.where(member, 1.0, 0.0).astype(BF), before, preferred_element_type=F32)
        chosen = member & (position == (row % 4).astype(F32)) & (lane // 8 == (row // 4) % 2)
        spread = jnp.where(chosen, jnp.where(first, w0, w1), 0.0).T
        coarse = spread.astype(BF)
        fine = (spread - coarse.astype(F32)).astype(BF)
        return jnp.concatenate([coarse[:16], fine[:16]], axis=0)

    def sum_straight():
        landed(near.at[0, pl.ds(1, 3)], n_r.at[0])
        landed(near.at[pl.ds(1, 3)], n_r.at[1])
        for ry in (2, 1, 3, 0):
            for n in range(0, half, step):
                both = jnp.dot(ymix[ry], near[:, :, ry, :, n : n + step].reshape(128, step), preferred_element_type=F32)
                total = both[:16] + both[16:]
                for m in range(2):
                    at = slice(2 * n + m * step, 2 * n + m * step + step)
                    if ry:
                        ysum[ry - 1, :, at] = total[8 * m : 8 * m + 8].astype(BF)
                    else:
                        yown[:, at] = total[8 * m : 8 * m + 8]
            if ry:
                remote(ysum.at[ry - 1], yret.at[NY - ry - 1], y_r.at[0], device(0, ry, 0), all_s.at[4])

    weight_parts(3)
    mix[...] = token_mix(xinfo[0], 1)
    spread_first()
    weight_parts(3)
    spread_on(0)
    spread_on(1)
    spread_own(3)
    spread_own(6)
    for load in loads:
        load.wait()
    arrived(0)
    for n, ref in enumerate((wg.at[:, far], wu.at[:, far], wd.at[far])):
        landed(ref, w_r.at[n])
    ffn_up(0)
    spread_on(2)
    spread_own(4)
    ffn_down(0)
    spread_on(3)
    go_back(0)
    spread_own(5)
    spread_own(7)
    arrived(1)
    ffn_up(1)
    spread_on(4)
    spread_on(6)
    spread_on(5)
    ffn_down(1)
    go_back(1)
    spread_on(7)
    landed(yinfo.at[pl.ds(1, 3)], j_r.at[0])
    ymix[0] = token_mix(xinfo[0], 0)
    for k in range(1, NY):
        ymix[k] = token_mix(yinfo[k], 0)
    arrived(2)
    ffn_up(2)
    down_and_reduce(2)
    reduce_first(2)
    arrived(3)
    ffn_up(3)
    down_and_reduce(3)
    reduce_on(2)
    reduce_first(3)
    finish(2)
    reduce_on(3)
    finish(3)
    sum_straight()

    landed(yret, y_r.at[0])
    landed(ret, b_r.at[0])
    for n in range(0, half, step):
        both = jnp.dot(mix[...], ret[:, :, :, n : n + step].reshape(128, step), preferred_element_type=F32)
        total = both[:16] + both[16:]
        for m in range(2):
            at = slice(2 * n + m * step, 2 * n + m * step + step)
            rest = yown[:, at]
            for k in range(NY - 1):
                rest = rest + yret[k, :, at].astype(F32)
            out_ref[:, at] = (total[8 * m : 8 * m + 8] + rest).astype(BF)
    for copy in sent[-POOL:]:
        copy.wait_send()
    for n, ref in enumerate((zback.at[0, 0, pl.ds(1, 3)], zback.at[0, 1], zback.at[1], zsum, ysum)):
        landed(ref, all_s.at[n])


def shards(tokens, expert_ids, route_weights, w_gate, w_up, w_down):
    block, width = tokens.shape
    hidden = w_gate.shape[2]
    dma = pltpu.SemaphoreType.DMA
    vmem = pl.BlockSpec(memory_space=pltpu.VMEM)
    hbm = pl.BlockSpec(memory_space=pl.ANY)
    return pl.pallas_call(
        kernel,
        out_shape=pltpu.VMEM((block, width), BF),
        in_specs=[hbm] * 6,
        out_specs=vmem,
        scratch_shapes=[
            pltpu.VMEM((NX, block, width), BF),
            pltpu.VMEM((NX, 8, 128), F32),
            pltpu.VMEM((2, 16, width), BF),
            pltpu.VMEM((GROUPS, 8, 16, width), BF),
            pltpu.VMEM((width, 2 * hidden), BF),
            pltpu.VMEM((width, 2 * hidden), BF),
            pltpu.VMEM((2 * hidden, width), BF),
            pltpu.VMEM((128, 2 * hidden), BF),
            pltpu.VMEM((GROUPS, 8, 16, width), BF),
            pltpu.VMEM((2, 2, 16, width), BF),
            pltpu.VMEM((2, 2, 2, 16, width), BF),
            pltpu.VMEM((2, 2, NX, 8, width // 2), BF),
            pltpu.VMEM((4, NX, 8, width // 2), BF),
            pltpu.VMEM((32, 128), BF),
            pltpu.VMEM((NY, 8, 128), F32),
            pltpu.VMEM((2, 2, NX, NY, 8, width // 2), BF),
            pltpu.VMEM((4, NX, NY, 8, width // 2), BF),
            pltpu.VMEM((NY, 32, 128), BF),
            pltpu.VMEM((3, block, width), BF),
            pltpu.VMEM((block, width), F32),
            pltpu.VMEM((3, block, width), BF),
            pltpu.VMEM((2, 8), jnp.int32),
            pltpu.VMEM((2, 8), F32),
            dma((POOL,)), dma((5,)),
            dma((2,)), dma((1,)),
            dma((11,)),
            dma((2, 11)), dma((4,)),
            dma((2, 2, 2)), dma((4, 2)),
            dma((1,)),
            dma((2,)),
            dma((1,)), dma((1,)),
            dma((3,)),
            dma((3,)), dma((3,)),
        ],
        compiler_params=pltpu.CompilerParams(
            collective_id=0, has_side_effects=True, vmem_limit_bytes=62 * 1024 * 1024
        ),
    )(tokens, expert_ids.T, route_weights.T, w_gate, w_up, w_down)


def solution(mesh):
    placed = (
        P(("expert", "shard"), None),
        P(("expert", "shard"), None),
        P(("expert", "shard"), None),
        P("expert", None, "shard"),
        P("expert", None, "shard"),
        P("expert", "shard", None),
    )
    return jax.shard_map(
        shards, mesh=mesh, in_specs=placed, out_specs=P(("expert", "shard"), None), check_vma=False
    )
```
